256 devices in a mesh: ctx: 64 (over x, z_hi, y, core), tp: 4 (over z_lo).
Axes of the slice: x: 4, y: 4, z: 8 (z_hi: 2, z_lo: 4; z = z_hi * 4 + z_lo), core: 2. Of those that a mesh axis runs over, the one named last changes fastest.
Arguments:
- queries: bfloat16 [8192, 32, 128], P('ctx', 'tp'), may hold values from -8 to 8
- window_keys: bfloat16 [8192, 4, 128], P('ctx', 'tp'), may hold values from -8 to 8
- window_values: bfloat16 [8192, 4, 128], P('ctx', 'tp'), may hold values from -6 to 6
- anchor_keys: bfloat16 [4096, 4, 128], P('ctx', 'tp'), may hold values from -8 to 8
- anchor_values: bfloat16 [4096, 4, 128], P('ctx', 'tp'), may hold values from -6 to 6
- passing_rows: int32 [64, 32], replicated, may hold values from 0 to 127, as said below
- block_of_device: int32 [64], replicated, may hold values from 0 to 63, each once
- out_weight: bfloat16 [4096, 4096], P(None, 'tp'), may hold values from -0.09375 to 0.09375
Outputs:
- mixed: bfloat16 [4096, 8192], P('tp', 'ctx')
The draws below stay inside these ranges and needn't reach their ends.
Inputs may be any that keep to these rules, and one draw needn't show every extreme that they name: `passing_rows`: each row holds 32 different positions. `block_of_device`: every block number appears once.
All inputs are finite; a program needn't handle non-finite values.
Results may differ from the reference program's by a relative error of at most 0.013.
Values may be sent and summed in bfloat16 or wider, within the bound.
A program may use at most 128 MiB of HBM per device.

```python
import jax
import jax.numpy as jnp
from jax import lax

HD = 128
QH = 32
KVH = 4
DOUT = 4096
TOK_DEV = 128
RETAIN = 32
NBLOCKS = 64
WINDOW = 8192
ANCHOR = 4096


def draw_queries(key, part):
    key_main = jax.random.fold_in(key, 17)
    values = jnp.clip(1.6 * jax.random.normal(key_main, (WINDOW, QH, HD)), -8.0, 8.0)
    return values.astype(jnp.bfloat16)


def draw_anchor_keys(key, part):
    key_main = jax.random.fold_in(key, 23)
    values = jnp.clip(1.6 * jax.random.normal(key_main, (ANCHOR, KVH, HD)), -8.0, 8.0)
    return values.astype(jnp.bfloat16)


def draw_passing_rows(key, part):
    row_keys = jax.random.split(jax.random.fold_in(key, 31), NBLOCKS)

    def one_row(row_key):
        return jax.random.permutation(row_key, TOK_DEV)[:RETAIN]
    return jax.vmap(one_row)(row_keys).astype(jnp.int32)


def shard_levels(key, extent, cuts, smallest, top_value):
    gain = 1.0
    for axis_at, parts in cuts:
        draws = jax.random.uniform(jax.random.fold_in(jax.random.fold_in(key, 6), axis_at), (parts,), jnp.float32, smallest / len(cuts), top_value / len(cuts))
        gain = gain * jnp.repeat(jnp.exp(draws), extent[axis_at] // parts).reshape((-1,) + (1,) * (len(extent) - 1 - axis_at))
    return gain


def scatter_about(key, shape, scale, bound, cuts=(), kind=jnp.bfloat16):
    array = scale * jax.random.normal(key, shape, jnp.float32)
    if cuts:
        array = array * shard_levels(key, shape, cuts, -0.22, 0.18)
    return jnp.clip(array, -bound, bound).astype(kind)


def setup_inputs(seed: int = 0) -> dict:
    key_of = jax.random.split(jax.random.key(seed), 9)
    queries = draw_queries(jax.random.fold_in(key_of[8], 71), 0)
    window_keys = scatter_about(key_of[1], (WINDOW, KVH, HD), 1.6, 8.0, ((0, 64), (1, 4)))
    window_values = scatter_about(key_of[2], (WINDOW, KVH, HD), 1.0, 6.0, ((0, 64), (1, 4)))
    anchor_keys = draw_anchor_keys(jax.random.fold_in(key_of[8], 71), 0)
    anchor_values = scatter_about(key_of[4], (ANCHOR, KVH, HD), 1.0, 6.0, ((0, 64), (1, 4)))
    passing_rows = draw_passing_rows(jax.random.fold_in(key_of[8], 71), 0)
    block_of_device = jax.random.permutation(key_of[6], NBLOCKS).astype(jnp.int32)
    out_weight = scatter_about(key_of[7], (DOUT, QH * HD), (QH * HD) ** -0.5, 0.09375, ((1, 4),))
    return {"queries": queries, "window_keys": window_keys, "window_values": window_values, "anchor_keys": anchor_keys, "anchor_values": anchor_values, "passing_rows": passing_rows, "block_of_device": block_of_device, "out_weight": out_weight}


def reference(queries, window_keys, window_values, anchor_keys, anchor_values, passing_rows, block_of_device, out_weight):
    blocks = block_of_device.shape[0]
    tok_rows = queries.shape[0] // blocks
    heads = queries.shape[1]
    kv_heads = window_keys.shape[1]
    head_size = queries.shape[2]
    group_size = heads // kv_heads
    retained = passing_rows.shape[1]
    offsets = jnp.arange(blocks, dtype=jnp.int32)[:, None] * tok_rows
    chosen = (passing_rows + offsets).reshape(-1).astype(jnp.int32)
    pass_keys = jnp.take(window_keys, chosen, axis=0)
    pass_values = jnp.take(window_values, chosen, axis=0)
    pass_blocks = jnp.repeat(block_of_device, retained)
    fixed_keys = jnp.concatenate([anchor_keys, pass_keys], axis=0).astype(jnp.float32)
    fixed_values = jnp.concatenate([anchor_values, pass_values], axis=0).astype(jnp.float32)
    anchor_count = anchor_keys.shape[0]
    fixed_count = fixed_keys.shape[0]
    places = jnp.arange(tok_rows, dtype=jnp.int32)
    causal = places[None, :] <= places[:, None]
    score_scale = head_size ** -0.5

    def one_block(slot_index):
        first_row = slot_index * tok_rows
        query_block = lax.dynamic_slice_in_dim(queries, first_row, tok_rows, 0).astype(jnp.float32)
        query_block = query_block.reshape(tok_rows, kv_heads, group_size, head_size)
        local_keys = lax.dynamic_slice_in_dim(window_keys, first_row, tok_rows, 0).astype(jnp.float32)
        local_values = lax.dynamic_slice_in_dim(window_values, first_row, tok_rows, 0).astype(jnp.float32)
        own_block = block_of_device[slot_index]
        fixed_seen = jnp.concatenate([jnp.ones((anchor_count,), dtype=bool), pass_blocks < own_block])
        visible = jnp.concatenate([jnp.broadcast_to(fixed_seen[None, :], (tok_rows, fixed_count)), causal], axis=1)
        key_rows = jnp.concatenate([fixed_keys, local_keys], axis=0)
        value_rows = jnp.concatenate([fixed_values, local_values], axis=0)
        scores = jnp.einsum('tgjd,ngd->tgjn', query_block, key_rows) * score_scale
        scores = jnp.where(visible[:, None, None, :], scores, -jnp.inf)
        row_max = jnp.max(scores, axis=-1, keepdims=True)
        weights = jnp.exp(scores - row_max)
        total = jnp.sum(weights, axis=-1)
        rounded = lax.optimization_barrier(weights.astype(jnp.bfloat16)).astype(jnp.float32)
        summed = jnp.einsum('tgjn,ngd->tgjd', rounded, value_rows) / total[..., None]
        return summed.reshape(tok_rows, heads * head_size).astype(jnp.bfloat16)

    attended = lax.map(one_block, jnp.arange(blocks, dtype=jnp.int32))
    attended = attended.reshape(blocks * tok_rows, heads * head_size)
    return jnp.dot(out_weight, attended.T, preferred_element_type=jnp.float32).astype(jnp.bfloat16)
```

```python
import math

import jax
import jax.numpy as jnp
from jax import lax
from jax.experimental import pallas as pl
from jax.experimental.pallas import tpu as pltpu
from jax.sharding import PartitionSpec as P

MESH = pl.DeviceIdType.MESH
RING = 4
HALVES = 2
F32 = jnp.float32
BF16 = jnp.bfloat16
NEG = -1e30
QB = 256
CHUNKS = 4


def kernel(
    wk_ref,
    wv_ref,
    ak_ref,
    av_ref,
    prt_ref,
    bod_ref,
    q_hbm,
    w_hbm,
    out_ref,
    g,
    q32,
    qh,
    w,
    m_ref,
    acc,
    vt,
    at,
    own,
    part,
    sbuf,
    rbuf,
    load_sem,
    gs_sem,
    gr_sem,
    ps_sem,
    pr_sem,
    ts_sem,
    tr_sem,
    tok,
    heads,
):
    anch = ak_ref.shape[0]
    ret = prt_ref.shape[0]
    keys = anch + ret
    hd = ak_ref.shape[1]
    half = keys
    ctx = lax.axis_index("ctx")
    tp = lax.axis_index("tp")
    core = lax.rem(ctx, 2)
    y = lax.rem(ctx // 2, RING)
    zh = lax.rem(ctx // (2 * RING), 2)
    x = ctx // (4 * RING)

    def slot_of(xx, zz, yy, cc):
        return ((xx * 2 + zz) * RING + yy) * 2 + cc

    def step_along(first, by):
        dx = core + first - 2 * core * first
        xx = lax.rem(x + (1 - dx) * by + RING, RING)
        yy = lax.rem(y + dx * by + RING, RING)
        return slot_of(xx, zh, yy, core)

    dev = {
        "f+": (step_along(0, 1), tp),
        "f-": (step_along(0, -1), tp),
        "s+": (step_along(1, 1), tp),
        "s-": (step_along(1, -1), tp),
        "z": (slot_of(x, 1 - zh, y, core), tp),
        "c": (slot_of(x, zh, y, 1 - core), tp),
    }

    q_load = pltpu.make_async_copy(q_hbm, q32, load_sem.at[0])
    w_load = pltpu.make_async_copy(w_hbm, w, load_sem.at[1])
    q_load.start()
    w_load.start()

    barrier = pltpu.get_barrier_semaphore()
    for d in dev.values():
        pl.semaphore_signal(barrier, inc=1, device_id=d, device_id_type=MESH)
    for k in range(1, 4):
        pl.semaphore_signal(
            barrier, inc=1, device_id=(ctx, lax.rem(tp + k, 4)), device_id_type=MESH
        )

    lane = lax.broadcasted_iota(jnp.int32, prt_ref.shape, 1)
    mine = jnp.where(lane == ctx, prt_ref[...], 0).astype(F32)
    chosen = jnp.sum(mine, axis=1, keepdims=True).astype(jnp.int32)
    pick = (lax.broadcasted_iota(jnp.int32, (ret, tok), 1) == chosen).astype(F32).astype(BF16)
    g[0, 0, 0, 0, 0:anch, :] = ak_ref[...]
    g[0, 0, 0, 0, keys : keys + anch, :] = av_ref[...]
    g[0, 0, 0, 0, anch:keys, :] = jnp.dot(
        pick, wk_ref[...], preferred_element_type=F32
    ).astype(BF16)
    g[0, 0, 0, 0, keys + anch : 2 * keys, :] = jnp.dot(
        pick, wv_ref[...], preferred_element_type=F32
    ).astype(BF16)

    pending = []
    count = [0]

    def remote(src, dst, recv, to):
        copy = pltpu.make_async_remote_copy(
            src_ref=src,
            dst_ref=dst,
            send_sem=gs_sem.at[count[0]],
            recv_sem=recv,
            device_id=dev[to],
            device_id_type=MESH,
        )
        count[0] += 1
        copy.start()
        pending.append(copy)

    def sem(z, d2, d1):
        return gr_sem.at[(z * RING + d2) * RING + d1]

    def arrived(z, d2, d1):
        ref = g.at[z, d2, 0, d1]
        if d2 == 0 and d1 == 2:
            for h in range(2):
                r = ref.at[pl.ds(h * half, half)]
                s = gr_sem.at[32 + z * 2 + h]
                pltpu.make_async_copy(r, r, s).wait()
        else:
            pltpu.make_async_copy(ref, ref, sem(z, d2, d1)).wait()

    def to_partner(z, d2, d1):
        remote(
            g.at[z, d2, 0, d1],
            g.at[z, d2, 1, d1],
            pr_sem.at[(z * RING + d2) * RING + d1],
            "c",
        )

    def second_both(z, d1):
        remote(g.at[z, 0, 0, d1], g.at[z, 3, 0, d1], sem(z, 3, d1), "s+")
        remote(g.at[z, 0, 0, d1], g.at[z, 1, 0, d1], sem(z, 1, d1), "s-")

    def start_own(z):
        remote(g.at[z, 0, 0, 0], g.at[z, 0, 0, 3], sem(z, 0, 3), "f+")
        remote(g.at[z, 0, 0, 0], g.at[z, 0, 0, 1], sem(z, 0, 1), "f-")
        second_both(z, 0)

    def after_first(z):
        for d1, to, h in ((3, "f+", 0), (1, "f-", 1)):
            arrived(z, 0, d1)
            rows = pl.ds(h * half, half)
            remote(
                g.at[z, 0, 0, d1, rows],
                g.at[z, 0, 0, 2, rows],
                gr_sem.at[32 + z * 2 + h],
                to,
            )
            second_both(z, d1)
            to_partner(z, 0, d1)

    def after_first_2(z):
        arrived(z, 0, 2)
        second_both(z, 2)
        to_partner(z, 0, 2)

    def after_second(z, d1):
        for d2, to in ((3, "s+"), (1, "s-")):
            arrived(z, d2, d1)
            if (d2 == 3) == (d1 in (0, 1)):
                remote(g.at[z, d2, 0, d1], g.at[z, 2, 0, d1], sem(z, 2, d1), to)
            to_partner(z, d2, d1)

    def after_second_2(z):
        for d1 in range(RING):
            arrived(z, 2, d1)
            to_partner(z, 2, d1)

    scale = (hd**-0.5) * math.log2(math.e)
    own_block = bod_ref[ctx]

    def fold(s, cols, n, first):
        top = jnp.max(s, axis=0, keepdims=True)
        if first:
            new = top
        else:
            old = m_ref[0:1, cols]
            new = jnp.maximum(old, top)
        p = jnp.exp2((s - new) * scale).astype(BF16)
        add = jnp.dot(vt[:, 0:n], p, preferred_element_type=F32)
        if first:
            acc[:, cols] = add
        else:
            acc[:, cols] = acc[:, cols] * jnp.exp2((old - new) * scale) + add
        m_ref[0:1, cols] = new

    def local_pass():
        vt[0:hd, 0:tok] = wv_ref[...].T
        row = lax.broadcasted_iota(jnp.int32, (tok, QB), 0)
        col = lax.broadcasted_iota(jnp.int32, (tok, QB), 1)
        seen = row <= lax.rem(col, tok)

        def block(i, c):
            cols = pl.ds(pl.multiple_of(i * QB, QB), QB)
            s = lax.dot_general(
                wk_ref[...], qh[cols, :], (((1,), (1,)), ((), ())), preferred_element_type=F32
            )
            fold(jnp.where(seen, s, NEG), cols, tok, True)
            return c

        lax.fori_loop(0, tok * heads // QB, block, 0)

    def compute(z, d2):
        for d1 in range(RING):
            r = g.at[z, d2, 1, d1]
            pltpu.make_async_copy(r, r, pr_sem.at[(z * RING + d2) * RING + d1]).wait()
        n = 2 * RING * keys
        vt[0:hd, 0:n] = g[z, d2, :, :, keys : 2 * keys, :].reshape(n, hd).T
        bias = []
        zz = zh if z == 0 else 1 - zh
        for s in range(2):
            cc = core if s == 0 else 1 - core
            for d1 in range(RING):
                dx = lax.rem(x + (1 - cc) * d1 + cc * d2, RING)
                dy = lax.rem(y + cc * d1 + (1 - cc) * d2, RING)
                bias.append(
                    jnp.where(bod_ref[slot_of(dx, zz, dy, cc)] < own_block, 0.0, NEG).astype(F32)
                )

        def block(i, c):
            cols = pl.ds(pl.multiple_of(i * QB, QB), QB)
            k = g[z, d2, :, :, 0:keys, :].reshape(n, hd)
            s = lax.dot_general(
                k, qh[cols, :], (((1,), (1,)), ((), ())), preferred_element_type=F32
            )
            parts = []
            for j in range(2 * RING):
                parts.append(s[j * keys : j * keys + anch])
                parts.append(s[j * keys + anch : (j + 1) * keys] + bias[j])
            fold(jnp.concatenate(parts, axis=0), cols, n, False)
            return c

        lax.fori_loop(0, tok * heads // QB, block, 0)

    pl.semaphore_wait(barrier, 9)
    start_own(0)
    remote(g.at[0, 0, 0, 0], g.at[1, 0, 0, 0], sem(1, 0, 0), "z")
    to_partner(0, 0, 0)

    q_load.wait()
    qh32 = q32[...].astype(F32)
    own[...] = qh32
    for h in range(heads):
        qh[h * tok : (h + 1) * tok, :] = own[pl.ds(h, tok, stride=heads), :].astype(BF16)
    vt[hd:, :] = jnp.ones((vt.shape[0] - hd, vt.shape[1]), BF16)
    local_pass()

    after_first(0)
    after_second(0, 0)
    after_first_2(0)
    after_second(0, 3)
    after_second(0, 1)
    compute(0, 0)
    arrived(1, 0, 0)
    start_own(1)
    to_partner(1, 0, 0)
    after_second(0, 2)
    after_first(1)
    after_second_2(0)
    compute(0, 1)
    after_second(1, 0)
    after_first_2(1)
    compute(0, 3)
    after_second(1, 3)
    after_second(1, 1)
    compute(0, 2)
    compute(1, 0)
    after_second(1, 2)
    compute(1, 1)
    after_second_2(1)
    compute(1, 3)
    compute(1, 2)

    for h in range(heads):
        cols = slice(h * tok, (h + 1) * tok)
        at[h * hd : (h + 1) * hd, :] = (
            acc[0:hd, cols] * (1.0 / acc[hd : hd + 1, cols])
        ).astype(BF16)

    side = tp // 2
    u = (1 - side) * tp + side * (3 - tp)

    def real(e):
        return (1 - side) * e + side * (3 - e)

    def pick2(edge, inner):
        return (1 - u) * edge + u * inner

    feats = out_ref.shape[0]
    rows = feats // CHUNKS
    w_load.wait()

    def product(e, ck):
        at_row = pl.multiple_of(e * feats + ck * rows, rows)
        return jnp.dot(w[pl.ds(at_row, rows), :], at[...], preferred_element_type=F32)

    def tp_copy(ph, ck, to, slot):
        r = pl.ds(pl.multiple_of(ck * rows, rows), rows)
        return pltpu.make_async_remote_copy(
            src_ref=sbuf.at[ph, r],
            dst_ref=rbuf.at[slot, r],
            send_sem=ts_sem.at[ph * CHUNKS + ck],
            recv_sem=tr_sem.at[slot * CHUNKS + ck],
            device_id=(ctx, to),
            device_id_type=MESH,
        )

    def landed(slot, ck):
        r = rbuf.at[slot, pl.ds(pl.multiple_of(ck * rows, rows), rows)]
        pltpu.make_async_copy(r, r, tr_sem.at[slot * CHUNKS + ck]).wait()

    plan = (
        (real(pick2(3, 2)), real(pick2(1, 2)), pick2(3, 1)),
        (real(pick2(2, 0)), real(pick2(2, 0)), pick2(2, 0)),
        (real(pick2(1, 3)), real(pick2(1, 3)), pick2(0, 1)),
    )

    def send_block(ph):
        e, to, slot = plan[ph]

        def one(ck, c):
            r = pl.ds(pl.multiple_of(ck * rows, rows), rows)
            if ph < 2:
                sbuf[ph, r, :] = product(e, ck).astype(BF16)
            else:
                part[...] = product(e, ck)

                @pl.when(u == 1)
                def _():
                    landed(3, ck)
                    part[...] += rbuf[3, r, :].astype(F32)

                sbuf[ph, r, :] = part[...].astype(BF16)
            tp_copy(ph, ck, to, slot).start()
            return c

        lax.fori_loop(0, CHUNKS, one, 0)

    send_block(0)
    send_block(1)

    def own_part(ck, c):
        r = pl.ds(pl.multiple_of(ck * rows, rows), rows)
        own[r, :] = product(tp, ck)
        return c

    lax.fori_loop(0, CHUNKS, own_part, 0)
    send_block(2)

    def finish(ck, c):
        r = pl.ds(pl.multiple_of(ck * rows, rows), rows)

        @pl.when(u == 1)
        def _():
            landed(2, ck)
            own[r, :] += rbuf[2, r, :].astype(F32)

        landed(0, ck)
        landed(1, ck)
        out_ref[r, :] = (
            own[r, :] + rbuf[0, r, :].astype(F32) + rbuf[1, r, :].astype(F32)
        ).astype(BF16)
        return c

    lax.fori_loop(0, CHUNKS, finish, 0)

    for copy in pending:
        copy.wait_send()
    for ph in range(3):
        e, to, slot = plan[ph]

        def drain(ck, c, ph=ph, to=to, slot=slot):
            tp_copy(ph, ck, to, slot).wait_send()
            return c

        lax.fori_loop(0, CHUNKS, drain, 0)


def body(
    queries,
    window_keys,
    window_values,
    anchor_keys,
    anchor_values,
    passing_rows,
    block_of_device,
    out_weight,
):
    tok, heads, hd = queries.shape
    anch = anchor_keys.shape[0]
    ret = passing_rows.shape[1]
    dout = out_weight.shape[0]
    feats = dout // lax.axis_size("tp")
    keys = anch + ret
    n = 2 * RING * keys
    vm = pl.BlockSpec(memory_space=pltpu.VMEM)
    sends = 2 * (4 + 12 + 16) + 1

    def run(*refs):
        kernel(*refs, tok=tok, heads=heads)

    return pl.pallas_call(
        run,
        out_shape=jax.ShapeDtypeStruct((feats, tok), BF16),
        in_specs=[vm] * 5
        + [
            pl.BlockSpec(memory_space=pltpu.SMEM),
            pl.BlockSpec(memory_space=pl.ANY),
            pl.BlockSpec(memory_space=pl.ANY),
        ],
        out_specs=vm,
        scratch_shapes=[
            pltpu.VMEM((HALVES, RING, 2, RING, 2 * keys, hd), BF16),
            pltpu.VMEM((tok * heads, hd), BF16),
            pltpu.VMEM((tok * heads, hd), BF16),
            pltpu.VMEM(out_weight.shape, BF16),
            pltpu.VMEM((8, tok * heads), F32),
            pltpu.VMEM((hd + 16, tok * heads), F32),
            pltpu.VMEM((hd + 16, n), BF16),
            pltpu.VMEM((heads * hd, tok), BF16),
            pltpu.VMEM((feats, tok), F32),
            pltpu.VMEM((feats // CHUNKS, tok), F32),
            pltpu.VMEM((3, feats, tok), BF16),
            pltpu.VMEM((4, feats, tok), BF16),
            pltpu.SemaphoreType.DMA((2,)),
            pltpu.SemaphoreType.DMA((sends,)),
            pltpu.SemaphoreType.DMA((36,)),
            pltpu.SemaphoreType.DMA((1,)),
            pltpu.SemaphoreType.DMA((32,)),
            pltpu.SemaphoreType.DMA((3 * CHUNKS,)),
            pltpu.SemaphoreType.DMA((4 * CHUNKS,)),
        ],
        compiler_params=pltpu.CompilerParams(collective_id=0, has_side_effects=True),
        name="layer",
    )(
        window_keys.reshape(tok, hd),
        window_values.reshape(tok, hd),
        anchor_keys.reshape(anch, hd),
        anchor_values.reshape(anch, hd),
        passing_rows.T,
        block_of_device,
        queries.reshape(tok * heads, hd),
        out_weight,
    )


def solution(mesh):
    return jax.shard_map(
        body,
        mesh=mesh,
        in_specs=(
            P("ctx", "tp", None),
            P("ctx", "tp", None),
            P("ctx", "tp", None),
            P("ctx", "tp", None),
            P("ctx", "tp", None),
            P(),
            P(),
            P(None, "tp"),
        ),
        out_specs=P("tp", "ctx"),
        check_vma=False,
    )
```

```python
import math

import jax
import jax.numpy as jnp
from jax import lax
from jax.experimental import pallas as pl
from jax.experimental.pallas import tpu as pltpu
from jax.sharding import PartitionSpec as P

MESH = pl.DeviceIdType.MESH
RING = 4
HALVES = 2
F32 = jnp.float32
BF16 = jnp.bfloat16
NEG = -1e30
QB = 256
CHUNKS = 4


def kernel(
    wk_hbm,
    wv_hbm,
    ak_hbm,
    av_hbm,
    prt_hbm,
    bod_hbm,
    q_hbm,
    w_hbm,
    out_ref,
    wk_ref,
    wv_ref,
    prt_ref,
    bod_ref,
    g,
    q32,
    qh,
    w,
    m_ref,
    acc,
    vt,
    at,
    own,
    part,
    sbuf,
    rbuf,
    load_sem,
    gs_sem,
    gr_sem,
    pr_sem,
    ts_sem,
    tr_sem,
    tok,
    heads,
):
    anch = ak_hbm.shape[0]
    ret = prt_ref.shape[0]
    keys = anch + ret
    hd = ak_hbm.shape[1]
    half = keys
    ctx = lax.axis_index("ctx")
    tp = lax.axis_index("tp")
    core = lax.rem(ctx, 2)
    y = lax.rem(ctx // 2, RING)
    zh = lax.rem(ctx // (2 * RING), 2)
    x = ctx // (4 * RING)

    def slot_of(xx, zz, yy, cc):
        return ((xx * 2 + zz) * RING + yy) * 2 + cc

    def step_along(first, by):
        dx = core + first - 2 * core * first
        xx = lax.rem(x + (1 - dx) * by + RING, RING)
        yy = lax.rem(y + dx * by + RING, RING)
        return slot_of(xx, zh, yy, core)

    dev = {
        "f+": (step_along(0, 1), tp),
        "f-": (step_along(0, -1), tp),
        "s+": (step_along(1, 1), tp),
        "s-": (step_along(1, -1), tp),
        "z": (slot_of(x, 1 - zh, y, core), tp),
        "c": (slot_of(x, zh, y, 1 - core), tp),
    }

    barrier = pltpu.get_barrier_semaphore()
    for d in dev.values():
        pl.semaphore_signal(barrier, inc=1, device_id=d, device_id_type=MESH)
    for k in range(1, 4):
        pl.semaphore_signal(
            barrier, inc=1, device_id=(ctx, lax.rem(tp + k, 4)), device_id_type=MESH
        )

    def load(k, src, dst):
        copy = pltpu.make_async_copy(src, dst, load_sem.at[k])
        copy.start()
        return copy

    prt_load = load(0, prt_hbm, prt_ref)
    wk_load = load(1, wk_hbm, wk_ref)
    wv_load = load(2, wv_hbm, wv_ref)
    ak_load = load(3, ak_hbm, g.at[0, 0, 0, 0, pl.ds(0, anch)])
    av_load = load(4, av_hbm, g.at[0, 0, 0, 0, pl.ds(keys, anch)])
    bod_load = load(5, bod_hbm, bod_ref)
    q_load = load(6, q_hbm, q32)
    w_load = load(7, w_hbm, w)

    prt_load.wait()
    lane = lax.broadcasted_iota(jnp.int32, prt_ref.shape, 1)
    mine = jnp.where(lane == ctx, prt_ref[...], 0).astype(F32)
    chosen = jnp.sum(mine, axis=1, keepdims=True).astype(jnp.int32)
    pick = (lax.broadcasted_iota(jnp.int32, (ret, tok), 1) == chosen).astype(F32).astype(BF16)
    wk_load.wait()
    wv_load.wait()
    g[0, 0, 0, 0, anch:keys, :] = jnp.dot(
        pick, wk_ref[...], preferred_element_type=F32
    ).astype(BF16)
    g[0, 0, 0, 0, keys + anch : 2 * keys, :] = jnp.dot(
        pick, wv_ref[...], preferred_element_type=F32
    ).astype(BF16)

    pending = []
    count = [0]

    def remote(src, dst, recv, to):
        copy = pltpu.make_async_remote_copy(
            src_ref=src,
            dst_ref=dst,
            send_sem=gs_sem.at[count[0]],
            recv_sem=recv,
            device_id=dev[to],
            device_id_type=MESH,
        )
        count[0] += 1
        copy.start()
        pending.append(copy)

    def sem(z, d2, d1):
        return gr_sem.at[(z * RING + d2) * RING + d1]

    def arrived(z, d2, d1):
        ref = g.at[z, d2, 0, d1]
        if d2 == 0 and d1 == 2:
            for h in range(2):
                r = ref.at[pl.ds(h * half, half)]
                s = gr_sem.at[32 + z * 2 + h]
                pltpu.make_async_copy(r, r, s).wait()
        else:
            pltpu.make_async_copy(ref, ref, sem(z, d2, d1)).wait()

    def to_partner(z, d2, d1):
        remote(
            g.at[z, d2, 0, d1],
            g.at[z, d2, 1, d1],
            pr_sem.at[(z * RING + d2) * RING + d1],
            "c",
        )

    def second_both(z, d1):
        remote(g.at[z, 0, 0, d1], g.at[z, 3, 0, d1], sem(z, 3, d1), "s+")
        remote(g.at[z, 0, 0, d1], g.at[z, 1, 0, d1], sem(z, 1, d1), "s-")

    def start_own(z):
        remote(g.at[z, 0, 0, 0], g.at[z, 0, 0, 3], sem(z, 0, 3), "f+")
        remote(g.at[z, 0, 0, 0], g.at[z, 0, 0, 1], sem(z, 0, 1), "f-")
        second_both(z, 0)

    def after_first(z):
        for d1, to, h in ((3, "f+", 0), (1, "f-", 1)):
            arrived(z, 0, d1)
            rows = pl.ds(h * half, half)
            remote(
                g.at[z, 0, 0, d1, rows],
                g.at[z, 0, 0, 2, rows],
                gr_sem.at[32 + z * 2 + h],
                to,
            )
            second_both(z, d1)
            to_partner(z, 0, d1)

    def after_first_2(z):
        arrived(z, 0, 2)
        second_both(z, 2)
        to_partner(z, 0, 2)

    def after_second(z, d1):
        for d2, to in ((3, "s+"), (1, "s-")):
            arrived(z, d2, d1)
            if (d2 == 3) == (d1 in (0, 1)):
                remote(g.at[z, d2, 0, d1], g.at[z, 2, 0, d1], sem(z, 2, d1), to)
            to_partner(z, d2, d1)

    def after_second_2(z):
        for d1 in range(RING):
            arrived(z, 2, d1)
            to_partner(z, 2, d1)

    scale = (hd**-0.5) * math.log2(math.e)
    ak_load.wait()
    av_load.wait()
    bod_load.wait()
    own_block = bod_ref[ctx]

    def fold(s, cols, n, first):
        top = jnp.max(s, axis=0, keepdims=True)
        if first:
            new = top
        else:
            old = m_ref[0:1, cols]
            new = jnp.maximum(old, top)
        p = jnp.exp2((s - new) * scale).astype(BF16)
        add = jnp.dot(vt[:, 0:n], p, preferred_element_type=F32)
        if first:
            acc[:, cols] = add
        else:
            acc[:, cols] = acc[:, cols] * jnp.exp2((old - new) * scale) + add
        m_ref[0:1, cols] = new

    def local_pass():
        vt[0:hd, 0:tok] = wv_ref[...].T
        row = lax.broadcasted_iota(jnp.int32, (tok, QB), 0)
        col = lax.broadcasted_iota(jnp.int32, (tok, QB), 1)
        seen = row <= lax.rem(col, tok)

        def scores(i):
            s = lax.dot_general(
                wk_ref[...],
                qh[i * QB : (i + 1) * QB, :],
                (((1,), (1,)), ((), ())),
                preferred_element_type=F32,
            )
            return jnp.where(seen, s, NEG)

        blocks = tok * heads // QB
        s = scores(0)
        for i in range(blocks):
            later = scores(i + 1) if i + 1 < blocks else None
            fold(s, slice(i * QB, (i + 1) * QB), tok, True)
            s = later

    def compute(z, d2):
        for d1 in range(RING):
            r = g.at[z, d2, 1, d1]
            pltpu.make_async_copy(r, r, pr_sem.at[(z * RING + d2) * RING + d1]).wait()
        n = 2 * RING * keys
        vt[0:hd, 0:n] = g[z, d2, :, :, keys : 2 * keys, :].reshape(n, hd).T
        bias = []
        zz = zh if z == 0 else 1 - zh
        for s in range(2):
            cc = core if s == 0 else 1 - core
            for d1 in range(RING):
                dx = lax.rem(x + (1 - cc) * d1 + cc * d2, RING)
                dy = lax.rem(y + cc * d1 + (1 - cc) * d2, RING)
                bias.append(
                    jnp.where(bod_ref[slot_of(dx, zz, dy, cc)] < own_block, 0.0, NEG).astype(F32)
                )

        def scores(i):
            k = g[z, d2, :, :, 0:keys, :].reshape(n, hd)
            s = lax.dot_general(
                k, qh[i * QB : (i + 1) * QB, :], (((1,), (1,)), ((), ())), preferred_element_type=F32
            )
            parts = []
            for j in range(2 * RING):
                parts.append(s[j * keys : j * keys + anch])
                parts.append(s[j * keys + anch : (j + 1) * keys] + bias[j])
            return jnp.concatenate(parts, axis=0)

        blocks = tok * heads // QB
        s = scores(0)
        for i in range(blocks):
            later = scores(i + 1) if i + 1 < blocks else None
            fold(s, slice(i * QB, (i + 1) * QB), n, False)
            s = later

    pl.semaphore_wait(barrier, 9)
    start_own(0)
    remote(g.at[0, 0, 0, 0], g.at[1, 0, 0, 0], sem(1, 0, 0), "z")
    to_partner(0, 0, 0)

    q_load.wait()
    qh32 = q32[...].astype(F32)
    own[...] = qh32
    for h in range(heads):
        qh[h * tok : (h + 1) * tok, :] = own[pl.ds(h, tok, stride=heads), :].astype(BF16)
    vt[hd:, :] = jnp.ones((vt.shape[0] - hd, vt.shape[1]), BF16)
    local_pass()

    after_first(0)
    after_second(0, 0)
    after_first_2(0)
    after_second(0, 3)
    after_second(0, 1)
    compute(0, 0)
    arrived(1, 0, 0)
    start_own(1)
    to_partner(1, 0, 0)
    after_second(0, 2)
    after_first(1)
    after_second_2(0)
    compute(0, 1)
    after_second(1, 0)
    after_first_2(1)
    compute(0, 3)
    after_second(1, 3)
    after_second(1, 1)
    compute(0, 2)
    compute(1, 0)
    after_second(1, 2)
    compute(1, 1)
    after_second_2(1)
    compute(1, 3)
    compute(1, 2)

    for h in range(heads):
        cols = slice(h * tok, (h + 1) * tok)
        at[h * hd : (h + 1) * hd, :] = (
            acc[0:hd, cols] * (1.0 / acc[hd : hd + 1, cols])
        ).astype(BF16)

    side = tp // 2
    u = (1 - side) * tp + side * (3 - tp)

    def real(e):
        return (1 - side) * e + side * (3 - e)

    def pick2(edge, inner):
        return (1 - u) * edge + u * inner

    feats = out_ref.shape[0]
    rows = feats // CHUNKS
    w_load.wait()

    def product(e, ck):
        at_row = pl.multiple_of(e * feats + ck * rows, rows)
        return jnp.dot(w[pl.ds(at_row, rows), :], at[...], preferred_element_type=F32)

    def tp_copy(ph, ck, to, slot):
        r = pl.ds(pl.multiple_of(ck * rows, rows), rows)
        return pltpu.make_async_remote_copy(
            src_ref=sbuf.at[ph, r],
            dst_ref=rbuf.at[slot, r],
            send_sem=ts_sem.at[ph * CHUNKS + ck],
            recv_sem=tr_sem.at[slot * CHUNKS + ck],
            device_id=(ctx, to),
            device_id_type=MESH,
        )

    def landed(slot, ck):
        r = rbuf.at[slot, pl.ds(pl.multiple_of(ck * rows, rows), rows)]
        pltpu.make_async_copy(r, r, tr_sem.at[slot * CHUNKS + ck]).wait()

    plan = (
        (real(pick2(3, 2)), real(pick2(1, 2)), pick2(3, 1)),
        (real(pick2(2, 0)), real(pick2(2, 0)), pick2(2, 0)),
        (real(pick2(1, 3)), real(pick2(1, 3)), pick2(0, 1)),
    )

    def send_block(ph):
        e, to, slot = plan[ph]

        def one(ck, c):
            r = pl.ds(pl.multiple_of(ck * rows, rows), rows)
            if ph < 2:
                sbuf[ph, r, :] = product(e, ck).astype(BF16)
            else:
                part[...] = product(e, ck)

                @pl.when(u == 1)
                def _():
                    landed(3, ck)
                    part[...] += rbuf[3, r, :].astype(F32)

                sbuf[ph, r, :] = part[...].astype(BF16)
            tp_copy(ph, ck, to, slot).start()
            return c

        lax.fori_loop(0, CHUNKS, one, 0)

    send_block(0)
    send_block(1)

    def own_part(ck, c):
        r = pl.ds(pl.multiple_of(ck * rows, rows), rows)
        own[r, :] = product(tp, ck)
        return c

    lax.fori_loop(0, CHUNKS, own_part, 0)
    send_block(2)

    def finish(ck, c):
        r = pl.ds(pl.multiple_of(ck * rows, rows), rows)

        @pl.when(u == 1)
        def _():
            landed(2, ck)
            own[r, :] += rbuf[2, r, :].astype(F32)

        landed(0, ck)
        landed(1, ck)
        out_ref[r, :] = (
            own[r, :] + rbuf[0, r, :].astype(F32) + rbuf[1, r, :].astype(F32)
        ).astype(BF16)
        return c

    lax.fori_loop(0, CHUNKS, finish, 0)

    for copy in pending:
        copy.wait_send()
    for ph in range(3):
        e, to, slot = plan[ph]

        def drain(ck, c, ph=ph, to=to, slot=slot):
            tp_copy(ph, ck, to, slot).wait_send()
            return c

        lax.fori_loop(0, CHUNKS, drain, 0)


def body(
    queries,
    window_keys,
    window_values,
    anchor_keys,
    anchor_values,
    passing_rows,
    block_of_device,
    out_weight,
):
    tok, heads, hd = queries.shape
    anch = anchor_keys.shape[0]
    ret = passing_rows.shape[1]
    dout = out_weight.shape[0]
    feats = dout // lax.axis_size("tp")
    keys = anch + ret
    n = 2 * RING * keys
    sends = 2 * (4 + 12 + 16) + 1

    def run(*refs):
        kernel(*refs, tok=tok, heads=heads)

    return pl.pallas_call(
        run,
        out_shape=jax.ShapeDtypeStruct((feats, tok), BF16),
        in_specs=[pl.BlockSpec(memory_space=pltpu.HBM)] * 8,
        out_specs=pl.BlockSpec(memory_space=pltpu.VMEM),
        scratch_shapes=[
            pltpu.VMEM((tok, hd), BF16),
            pltpu.VMEM((tok, hd), BF16),
            pltpu.VMEM((ret, passing_rows.shape[0]), jnp.int32),
            pltpu.SMEM(block_of_device.shape, jnp.int32),
            pltpu.VMEM((HALVES, RING, 2, RING, 2 * keys, hd), BF16),
            pltpu.VMEM((tok * heads, hd), BF16),
            pltpu.VMEM((tok * heads, hd), BF16),
            pltpu.VMEM(out_weight.shape, BF16),
            pltpu.VMEM((8, tok * heads), F32),
            pltpu.VMEM((hd + 16, tok * heads), F32),
            pltpu.VMEM((hd + 16, n), BF16),
            pltpu.VMEM((heads * hd, tok), BF16),
            pltpu.VMEM((feats, tok), F32),
            pltpu.VMEM((feats // CHUNKS, tok), F32),
            pltpu.VMEM((3, feats, tok), BF16),
            pltpu.VMEM((4, feats, tok), BF16),
            pltpu.SemaphoreType.DMA((8,)),
            pltpu.SemaphoreType.DMA((sends,)),
            pltpu.SemaphoreType.DMA((36,)),
            pltpu.SemaphoreType.DMA((32,)),
            pltpu.SemaphoreType.DMA((3 * CHUNKS,)),
            pltpu.SemaphoreType.DMA((4 * CHUNKS,)),
        ],
        compiler_params=pltpu.CompilerParams(
            collective_id=0, has_side_effects=True, vmem_limit_bytes=56_000_000
        ),
        name="layer",
    )(
        *[
            pltpu.with_memory_space_constraint(a, pltpu.HBM)
            for a in (
                window_keys.reshape(tok, hd),
                window_values.reshape(tok, hd),
                anchor_keys.reshape(anch, hd),
                anchor_values.reshape(anch, hd),
                passing_rows.T,
                block_of_device,
                queries.reshape(tok * heads, hd),
                out_weight,
            )
        ]
    )


def solution(mesh):
    return jax.shard_map(
        body,
        mesh=mesh,
        in_specs=(
            P("ctx", "tp", None),
            P("ctx", "tp", None),
            P("ctx", "tp", None),
            P("ctx", "tp", None),
            P("ctx", "tp", None),
            P(),
            P(),
            P(None, "tp"),
        ),
        out_specs=P("tp", "ctx"),
        check_vma=False,
    )
```

```python
import math

import jax
import jax.numpy as jnp
from jax import lax
from jax.experimental import pallas as pl
from jax.experimental.pallas import tpu as pltpu
from jax.sharding import PartitionSpec as P

MESH = pl.DeviceIdType.MESH
RING = 4
HALVES = 2
F32 = jnp.float32
BF16 = jnp.bfloat16
NEG = -1e30
QB = 512
CHUNKS = 4
DIRECT = ((2,), (2,))


def kernel(
    wk_hbm,
    wv_hbm,
    ak_hbm,
    av_hbm,
    prt_hbm,
    bod_hbm,
    q_hbm,
    w_hbm,
    out_ref,
    wk_ref,
    wv_ref,
    prt_ref,
    bod_ref,
    g,
    q32,
    qh,
    w,
    m_ref,
    acc,
    vt,
    at,
    own,
    part,
    sbuf,
    rbuf,
    load_sem,
    gs_sem,
    gr_sem,
    pr_sem,
    ts_sem,
    tr_sem,
    tok,
    heads,
):
    anch = ak_hbm.shape[0]
    ret = prt_ref.shape[0]
    keys = anch + ret
    hd = ak_hbm.shape[1]
    ctx = lax.axis_index("ctx")
    tp = lax.axis_index("tp")
    core = lax.rem(ctx, 2)
    y = lax.rem(ctx // 2, RING)
    zh = lax.rem(ctx // (2 * RING), 2)
    x = ctx // (4 * RING)

    def spot(z, d2, s, d1):
        return ((z * RING + d2) * 2 + s) * RING + d1

    def slot_of(xx, zz, yy, cc):
        return ((xx * 2 + zz) * RING + yy) * 2 + cc

    def step_along(first, by):
        dx = core + first - 2 * core * first
        xx = lax.rem(x + (1 - dx) * by + RING, RING)
        yy = lax.rem(y + dx * by + RING, RING)
        return slot_of(xx, zh, yy, core)

    dev = {
        "f+": (step_along(0, 1), tp),
        "f-": (step_along(0, -1), tp),
        "f2": (step_along(0, 2), tp),
        "s+": (step_along(1, 1), tp),
        "s-": (step_along(1, -1), tp),
        "s2": (step_along(1, 2), tp),
        "z": (slot_of(x, 1 - zh, y, core), tp),
        "c": (slot_of(x, zh, y, 1 - core), tp),
    }

    barrier = pltpu.get_barrier_semaphore()
    for d in dev.values():
        pl.semaphore_signal(barrier, inc=1, device_id=d, device_id_type=MESH)
    for k in range(1, 4):
        pl.semaphore_signal(
            barrier, inc=1, device_id=(ctx, lax.rem(tp + k, 4)), device_id_type=MESH
        )

    def load(k, src, dst):
        copy = pltpu.make_async_copy(src, dst, load_sem.at[k])
        copy.start()
        return copy

    prt_load = load(0, prt_hbm, prt_ref)
    wk_load = load(1, wk_hbm, wk_ref)
    wv_load = load(2, wv_hbm, wv_ref)
    ak_load = load(3, ak_hbm, g.at[0, pl.ds(0, anch)])
    av_load = load(4, av_hbm, g.at[0, pl.ds(keys, anch)])
    bod_load = load(5, bod_hbm, bod_ref)
    q_load = load(6, q_hbm, q32)
    w_load = load(7, w_hbm, w)

    prt_load.wait()
    lane = lax.broadcasted_iota(jnp.int32, prt_ref.shape, 1)
    mine = jnp.where(lane == ctx, prt_ref[...], 0).astype(F32)
    chosen = jnp.sum(mine, axis=1, keepdims=True).astype(jnp.int32)
    pick = (lax.broadcasted_iota(jnp.int32, (ret, tok), 1) == chosen).astype(F32).astype(BF16)
    wk_load.wait()
    wv_load.wait()
    g[0, anch:keys, :] = jnp.dot(
        pick, wk_ref[...], preferred_element_type=F32
    ).astype(BF16)
    g[0, keys + anch : 2 * keys, :] = jnp.dot(
        pick, wv_ref[...], preferred_element_type=F32
    ).astype(BF16)

    sent = []

    def remote(src, dst, recv, to):
        copy = pltpu.make_async_remote_copy(
            src_ref=src,
            dst_ref=dst,
            send_sem=gs_sem,
            recv_sem=recv,
            device_id=dev[to],
            device_id_type=MESH,
        )
        copy.start()
        sent.append(1)

    def sem(z, d2, d1):
        return gr_sem.at[z * 13 + (12 if d2 == 2 else d1 + (0, 4, 0, 8)[d2])]

    def arrived(z, d2, d1):
        ref = g.at[spot(z, d2, 0, d1)]
        pltpu.make_async_copy(ref, ref, sem(z, d2, d1)).wait()

    def to_partner(z, d2, d1):
        remote(
            g.at[spot(z, d2, 0, d1)],
            g.at[spot(z, d2, 1, d1)],
            pr_sem.at[z * RING + d2],
            "c",
        )

    def second_all(z, d1):
        own = g.at[spot(z, 0, 0, d1)]
        remote(own, g.at[spot(z, 3, 0, d1)], sem(z, 3, d1), "s+")
        remote(own, g.at[spot(z, 1, 0, d1)], sem(z, 1, d1), "s-")
        if d1 in DIRECT[z]:
            remote(own, g.at[spot(z, 2, 0, d1)], sem(z, 2, d1), "s2")

    def start_own(z):
        own = g.at[spot(z, 0, 0, 0)]
        remote(own, g.at[spot(z, 0, 0, 3)], sem(z, 0, 3), "f+")
        remote(own, g.at[spot(z, 0, 0, 1)], sem(z, 0, 1), "f-")
        remote(own, g.at[spot(z, 0, 0, 2)], sem(z, 0, 2), "f2")
        second_all(z, 0)
        to_partner(z, 0, 0)

    def after_first(z, d1):
        arrived(z, 0, d1)
        second_all(z, d1)
        to_partner(z, 0, d1)

    def after_second(z, d1):
        for d2, to in ((3, "s+"), (1, "s-")):
            arrived(z, d2, d1)
            if d1 not in DIRECT[z] and (d2 == 3) == (d1 in (0, 2)):
                remote(g.at[spot(z, d2, 0, d1)], g.at[spot(z, 2, 0, d1)], sem(z, 2, d1), to)
            to_partner(z, d2, d1)

    def whole_row(z, d2, s, arrival):
        r = g.at[pl.ds(spot(z, d2, s, 0), RING)]
        pltpu.make_async_copy(r, r, arrival).wait()

    def after_second_2(z):
        whole_row(z, 2, 0, sem(z, 2, 0))
        for d1 in range(RING):
            to_partner(z, 2, d1)

    scale = (hd**-0.5) * math.log2(math.e)
    ak_load.wait()
    av_load.wait()
    bod_load.wait()
    own_block = bod_ref[ctx]

    def fold(s, cols, n, first):
        top = jnp.max(s, axis=0, keepdims=True)
        if first:
            new = top
        else:
            old = m_ref[0:1, cols]
            new = jnp.maximum(old, top)
        p = jnp.exp2((s - new) * scale).astype(BF16)
        add = jnp.dot(vt[:, 0:n], p, preferred_element_type=F32)
        if first:
            acc[:, cols] = add
        else:
            acc[:, cols] = acc[:, cols] * jnp.exp2((old - new) * scale) + add
        m_ref[0:1, cols] = new

    def local_pass():
        vt[0:hd, 0:tok] = wv_ref[...].T
        row = lax.broadcasted_iota(jnp.int32, (tok, QB), 0)
        col = lax.broadcasted_iota(jnp.int32, (tok, QB), 1)
        seen = row <= lax.rem(col, tok)

        def scores(i):
            s = lax.dot_general(
                wk_ref[...],
                qh[i * QB : (i + 1) * QB, :],
                (((1,), (1,)), ((), ())),
                preferred_element_type=F32,
            )
            return jnp.where(seen, s, NEG)

        blocks = tok * heads // QB
        s = scores(0)
        for i in range(blocks):
            later = scores(i + 1) if i + 1 < blocks else None
            fold(s, slice(i * QB, (i + 1) * QB), tok, True)
            s = later

    def compute(*units):
        n = len(units) * RING * keys
        bias = []
        for k, (z, d2, s) in enumerate(units):
            if s == 1:
                whole_row(z, d2, 1, pr_sem.at[z * RING + d2])
            at_col = k * RING * keys
            vt[0:hd, at_col : at_col + RING * keys] = (
                g[spot(z, d2, s, 0) : spot(z, d2, s, 0) + RING, keys : 2 * keys, :].reshape(RING * keys, hd).T
            )
            zz = zh if z == 0 else 1 - zh
            cc = core if s == 0 else 1 - core
            for d1 in range(RING):
                dx = lax.rem(x + (1 - cc) * d1 + cc * d2, RING)
                dy = lax.rem(y + cc * d1 + (1 - cc) * d2, RING)
                bias.append(
                    jnp.where(bod_ref[slot_of(dx, zz, dy, cc)] < own_block, 0.0, NEG).astype(F32)
                )

        def scores(i):
            k = jnp.concatenate(
                [
                    g[spot(z, d2, s, 0) : spot(z, d2, s, 0) + RING, 0:keys, :].reshape(RING * keys, hd)
                    for z, d2, s in units
                ],
                axis=0,
            )
            s = lax.dot_general(
                k, qh[i * QB : (i + 1) * QB, :], (((1,), (1,)), ((), ())), preferred_element_type=F32
            )
            parts = []
            for j in range(len(bias)):
                parts.append(s[j * keys : j * keys + anch])
                parts.append(s[j * keys + anch : (j + 1) * keys] + bias[j])
            return jnp.concatenate(parts, axis=0)

        blocks = tok * heads // QB
        s = scores(0)
        for i in range(blocks):
            later = scores(i + 1) if i + 1 < blocks else None
            fold(s, slice(i * QB, (i + 1) * QB), n, False)
            s = later

    pl.semaphore_wait(barrier, 11)
    remote(g.at[spot(0, 0, 0, 0)], g.at[spot(1, 0, 0, 0)], sem(1, 0, 0), "z")
    start_own(0)

    q_load.wait()
    own[...] = q32[...].astype(F32)
    for h in range(heads):
        qh[h * tok : (h + 1) * tok, :] = own[pl.ds(h, tok, stride=heads), :].astype(BF16)
    vt[hd:, :] = jnp.ones((vt.shape[0] - hd, vt.shape[1]), BF16)
    local_pass()

    after_first(0, 3)
    after_first(0, 1)
    after_second(0, 0)
    after_first(0, 2)
    arrived(1, 0, 0)
    start_own(1)
    compute((0, 0, 0))
    after_second(0, 3)
    after_second(0, 1)
    after_second(0, 2)
    after_first(1, 3)
    after_first(1, 1)
    compute((0, 1, 0), (0, 0, 1))
    after_second(1, 0)
    after_first(1, 2)
    after_second_2(0)
    compute((0, 3, 0), (0, 1, 1))
    after_second(1, 3)
    after_second(1, 1)
    compute((1, 0, 0), (0, 3, 1))
    after_second(1, 2)
    compute((0, 2, 0), (1, 0, 1))
    compute((1, 1, 0), (0, 2, 1))
    after_second_2(1)
    compute((1, 3, 0), (1, 1, 1))
    compute((1, 2, 0), (1, 3, 1))
    compute((1, 2, 1))

    for h in range(heads):
        cols = slice(h * tok, (h + 1) * tok)
        at[h * hd : (h + 1) * hd, :] = (
            acc[0:hd, cols] * (1.0 / acc[hd : hd + 1, cols])
        ).astype(BF16)

    side = tp // 2
    u = (1 - side) * tp + side * (3 - tp)

    def real(e):
        return (1 - side) * e + side * (3 - e)

    def pick2(edge, inner):
        return (1 - u) * edge + u * inner

    feats = out_ref.shape[0]
    rows = feats // CHUNKS
    w_load.wait()

    def product(e, ck):
        at_row = pl.multiple_of(e * feats + ck * rows, rows)
        return jnp.dot(w[pl.ds(at_row, rows), :], at[...], preferred_element_type=F32)

    def tp_copy(ph, ck, to, slot):
        r = pl.ds(pl.multiple_of(ck * rows, rows), rows)
        return pltpu.make_async_remote_copy(
            src_ref=sbuf.at[ph, r],
            dst_ref=rbuf.at[slot, r],
            send_sem=ts_sem,
            recv_sem=tr_sem.at[slot * CHUNKS + ck],
            device_id=(ctx, to),
            device_id_type=MESH,
        )

    def landed(slot, ck):
        r = rbuf.at[slot, pl.ds(pl.multiple_of(ck * rows, rows), rows)]
        pltpu.make_async_copy(r, r, tr_sem.at[slot * CHUNKS + ck]).wait()

    plan = (
        (real(pick2(3, 2)), real(pick2(1, 2)), pick2(3, 1)),
        (real(pick2(2, 0)), real(pick2(2, 0)), pick2(2, 0)),
        (real(pick2(1, 3)), real(pick2(1, 3)), pick2(0, 1)),
    )

    def send_block(ph):
        e, to, slot = plan[ph]

        def one(ck, c):
            r = pl.ds(pl.multiple_of(ck * rows, rows), rows)
            if ph < 2:
                sbuf[ph, r, :] = product(e, ck).astype(BF16)
            else:
                part[...] = product(e, ck)

                @pl.when(u == 1)
                def _():
                    landed(3, ck)
                    part[...] += rbuf[3, r, :].astype(F32)

                sbuf[ph, r, :] = part[...].astype(BF16)
            tp_copy(ph, ck, to, slot).start()
            return c

        lax.fori_loop(0, CHUNKS, one, 0)

    send_block(0)
    send_block(1)

    def own_part(ck, c):
        r = pl.ds(pl.multiple_of(ck * rows, rows), rows)
        own[r, :] = product(tp, ck)
        return c

    lax.fori_loop(0, CHUNKS, own_part, 0)
    send_block(2)

    def finish(ck, c):
        r = pl.ds(pl.multiple_of(ck * rows, rows), rows)

        @pl.when(u == 1)
        def _():
            landed(2, ck)
            own[r, :] += rbuf[2, r, :].astype(F32)

        landed(0, ck)
        landed(1, ck)
        out_ref[r, :] = (
            own[r, :] + rbuf[0, r, :].astype(F32) + rbuf[1, r, :].astype(F32)
        ).astype(BF16)
        return c

    lax.fori_loop(0, CHUNKS, finish, 0)

    def drain_all():
        gone = g.at[pl.ds(0, len(sent))]
        pltpu.make_async_copy(gone, gone, gs_sem).wait()
        pltpu.make_async_copy(sbuf, sbuf, ts_sem).wait()

    drain_all()


def body(
    queries,
    window_keys,
    window_values,
    anchor_keys,
    anchor_values,
    passing_rows,
    block_of_device,
    out_weight,
):
    tok, heads, hd = queries.shape
    anch = anchor_keys.shape[0]
    ret = passing_rows.shape[1]
    dout = out_weight.shape[0]
    feats = dout // lax.axis_size("tp")
    keys = anch + ret
    n = 2 * RING * keys

    def run(*refs):
        kernel(*refs, tok=tok, heads=heads)

    return pl.pallas_call(
        run,
        out_shape=jax.ShapeDtypeStruct((feats, tok), BF16),
        in_specs=[pl.BlockSpec(memory_space=pltpu.HBM)] * 8,
        out_specs=pl.BlockSpec(memory_space=pltpu.VMEM),
        scratch_shapes=[
            pltpu.VMEM((tok, hd), BF16),
            pltpu.VMEM((tok, hd), BF16),
            pltpu.VMEM((ret, passing_rows.shape[0]), jnp.int32),
            pltpu.SMEM(block_of_device.shape, jnp.int32),
            pltpu.VMEM((HALVES * RING * 2 * RING, 2 * keys, hd), BF16),
            pltpu.VMEM((tok * heads, hd), BF16),
            pltpu.VMEM((tok * heads, hd), BF16),
            pltpu.VMEM(out_weight.shape, BF16),
            pltpu.VMEM((8, tok * heads), F32),
            pltpu.VMEM((hd + 16, tok * heads), F32),
            pltpu.VMEM((hd + 16, n), BF16),
            pltpu.VMEM((heads * hd, tok), BF16),
            pltpu.VMEM((feats, tok), F32),
            pltpu.VMEM((feats // CHUNKS, tok), F32),
            pltpu.VMEM((3, feats, tok), BF16),
            pltpu.VMEM((4, feats, tok), BF16),
            pltpu.SemaphoreType.DMA((8,)),
            pltpu.SemaphoreType.DMA,
            pltpu.SemaphoreType.DMA((26,)),
            pltpu.SemaphoreType.DMA((2 * RING,)),
            pltpu.SemaphoreType.DMA,
            pltpu.SemaphoreType.DMA((4 * CHUNKS,)),
        ],
        compiler_params=pltpu.CompilerParams(
            collective_id=0, has_side_effects=True, vmem_limit_bytes=56_000_000
        ),
        name="layer",
    )(
        *[
            pltpu.with_memory_space_constraint(a, pltpu.HBM)
            for a in (
                window_keys.reshape(tok, hd),
                window_values.reshape(tok, hd),
                anchor_keys.reshape(anch, hd),
                anchor_values.reshape(anch, hd),
                passing_rows.T,
                block_of_device,
                queries.reshape(tok * heads, hd),
                out_weight,
            )
        ]
    )


def solution(mesh):
    return jax.shard_map(
        body,
        mesh=mesh,
        in_specs=(
            P("ctx", "tp", None),
            P("ctx", "tp", None),
            P("ctx", "tp", None),
            P("ctx", "tp", None),
            P("ctx", "tp", None),
            P(),
            P(),
            P(None, "tp"),
        ),
        out_specs=P("tp", "ctx"),
        check_vma=False,
    )
```

```python
import math

import jax
import jax.numpy as jnp
from jax import lax
from jax.experimental import pallas as pl
from jax.experimental.pallas import tpu as pltpu
from jax.sharding import PartitionSpec as P

MESH = pl.DeviceIdType.MESH
RING = 4
HALVES = 2
F32 = jnp.float32
BF16 = jnp.bfloat16
NEG = -1e30
QB = 512
CHUNKS = 4
DIRECT = ((2,), (2,))


def kernel(
    wk_hbm,
    wv_hbm,
    ak_hbm,
    av_hbm,
    prt_hbm,
    bod_hbm,
    q_hbm,
    w_hbm,
    out_ref,
    wk_ref,
    wv_ref,
    prt_ref,
    bod_ref,
    g,
    q32,
    qh,
    w,
    m_ref,
    acc,
    vt,
    at,
    own,
    part,
    sbuf,
    rbuf,
    load_sem,
    gs_sem,
    gr_sem,
    pr_sem,
    ts_sem,
    tr_sem,
    tok,
    heads,
):
    anch = ak_hbm.shape[0]
    ret = prt_ref.shape[0]
    keys = anch + ret
    hd = ak_hbm.shape[1]
    ctx = lax.axis_index("ctx")
    tp = lax.axis_index("tp")
    core = lax.rem(ctx, 2)
    y = lax.rem(ctx // 2, RING)
    zh = lax.rem(ctx // (2 * RING), 2)
    x = ctx // (4 * RING)

    def spot(z, d2, s, d1):
        return ((z * RING + d2) * 2 + s) * RING + d1

    def slot_of(xx, zz, yy, cc):
        return ((xx * 2 + zz) * RING + yy) * 2 + cc

    def step_along(first, by):
        dx = core + first - 2 * core * first
        xx = lax.rem(x + (1 - dx) * by + RING, RING)
        yy = lax.rem(y + dx * by + RING, RING)
        return slot_of(xx, zh, yy, core)

    dev = {
        "f+": (step_along(0, 1), tp),
        "f-": (step_along(0, -1), tp),
        "f2": (step_along(0, 2), tp),
        "s+": (step_along(1, 1), tp),
        "s-": (step_along(1, -1), tp),
        "s2": (step_along(1, 2), tp),
        "z": (slot_of(x, 1 - zh, y, core), tp),
        "c": (slot_of(x, zh, y, 1 - core), tp),
    }

    barrier = pltpu.get_barrier_semaphore()
    for d in dev.values():
        pl.semaphore_signal(barrier, inc=1, device_id=d, device_id_type=MESH)
    for k in range(1, 4):
        pl.semaphore_signal(
            barrier, inc=1, device_id=(ctx, lax.rem(tp + k, 4)), device_id_type=MESH
        )

    def load(k, src, dst):
        copy = pltpu.make_async_copy(src, dst, load_sem.at[k])
        copy.start()
        return copy

    prt_load = load(0, prt_hbm, prt_ref)
    wk_load = load(1, wk_hbm, wk_ref)
    wv_load = load(2, wv_hbm, wv_ref)
    ak_load = load(3, ak_hbm, g.at[0, pl.ds(0, anch)])
    av_load = load(4, av_hbm, g.at[0, pl.ds(keys, anch)])
    bod_load = load(5, bod_hbm, bod_ref)
    q_load = load(6, q_hbm, q32)
    w_load = load(7, w_hbm, w)

    prt_load.wait()
    lane = lax.broadcasted_iota(jnp.int32, prt_ref.shape, 1)
    mine = jnp.where(lane == ctx, prt_ref[...], 0).astype(F32)
    chosen = jnp.sum(mine, axis=1, keepdims=True).astype(jnp.int32)
    pick = (lax.broadcasted_iota(jnp.int32, (ret, tok), 1) == chosen).astype(F32).astype(BF16)
    wk_load.wait()
    wv_load.wait()
    g[0, anch:keys, :] = jnp.dot(
        pick, wk_ref[...], preferred_element_type=F32
    ).astype(BF16)
    g[0, keys + anch : 2 * keys, :] = jnp.dot(
        pick, wv_ref[...], preferred_element_type=F32
    ).astype(BF16)

    sent = []

    def remote(src, dst, recv, to):
        copy = pltpu.make_async_remote_copy(
            src_ref=src,
            dst_ref=dst,
            send_sem=gs_sem,
            recv_sem=recv,
            device_id=dev[to],
            device_id_type=MESH,
        )
        copy.start()
        sent.append(1)

    def sem(z, d2, d1):
        return gr_sem.at[z * 13 + (12 if d2 == 2 else d1 + (0, 4, 0, 8)[d2])]

    def arrived(z, d2, d1):
        ref = g.at[spot(z, d2, 0, d1)]
        pltpu.make_async_copy(ref, ref, sem(z, d2, d1)).wait()

    def to_partner(z, d2, d1):
        remote(
            g.at[spot(z, d2, 0, d1)],
            g.at[spot(z, d2, 1, d1)],
            pr_sem.at[z * RING + d2],
            "c",
        )

    def second_all(z, d1):
        own = g.at[spot(z, 0, 0, d1)]
        remote(own, g.at[spot(z, 3, 0, d1)], sem(z, 3, d1), "s+")
        remote(own, g.at[spot(z, 1, 0, d1)], sem(z, 1, d1), "s-")
        if d1 in DIRECT[z]:
            remote(own, g.at[spot(z, 2, 0, d1)], sem(z, 2, d1), "s2")

    def start_own(z):
        own = g.at[spot(z, 0, 0, 0)]
        remote(own, g.at[spot(z, 0, 0, 3)], sem(z, 0, 3), "f+")
        remote(own, g.at[spot(z, 0, 0, 1)], sem(z, 0, 1), "f-")
        remote(own, g.at[spot(z, 0, 0, 2)], sem(z, 0, 2), "f2")
        second_all(z, 0)
        to_partner(z, 0, 0)

    def after_first(z, d1):
        arrived(z, 0, d1)
        second_all(z, d1)
        to_partner(z, 0, d1)

    def after_second(z, d1):
        for d2, to in ((3, "s+"), (1, "s-")):
            arrived(z, d2, d1)
            if d1 not in DIRECT[z] and (d2 == 3) == (d1 in (0, 2)):
                remote(g.at[spot(z, d2, 0, d1)], g.at[spot(z, 2, 0, d1)], sem(z, 2, d1), to)
            to_partner(z, d2, d1)

    def whole_row(z, d2, s, arrival):
        r = g.at[pl.ds(spot(z, d2, s, 0), RING)]
        pltpu.make_async_copy(r, r, arrival).wait()

    def after_second_2(z):
        whole_row(z, 2, 0, sem(z, 2, 0))
        for d1 in range(RING):
            to_partner(z, 2, d1)

    scale = (hd**-0.5) * math.log2(math.e)
    ak_load.wait()
    av_load.wait()
    bod_load.wait()
    own_block = bod_ref[ctx]

    def fold(s, cols, n, first):
        top = jnp.max(s, axis=0, keepdims=True)
        if first:
            new = top
        else:
            old = m_ref[0:1, cols]
            new = jnp.maximum(old, top)
        p = jnp.exp2((s - new) * scale).astype(BF16)
        add = jnp.dot(vt[:, 0:n], p, preferred_element_type=F32)
        if first:
            acc[:, cols] = add
        else:
            acc[:, cols] = acc[:, cols] * jnp.exp2((old - new) * scale) + add
        m_ref[0:1, cols] = new

    def local_pass():
        vt[0:hd, 0:tok] = wv_ref[...].T
        row = lax.broadcasted_iota(jnp.int32, (tok, QB), 0)
        col = lax.broadcasted_iota(jnp.int32, (tok, QB), 1)
        seen = row <= lax.rem(col, tok)

        def scores(i):
            s = lax.dot_general(
                wk_ref[...],
                qh[i * QB : (i + 1) * QB, :],
                (((1,), (1,)), ((), ())),
                preferred_element_type=F32,
            )
            return jnp.where(seen, s, NEG)

        blocks = tok * heads // QB
        s = scores(0)
        for i in range(blocks):
            later = scores(i + 1) if i + 1 < blocks else None
            fold(s, slice(i * QB, (i + 1) * QB), tok, True)
            s = later

    def compute(*units):
        n = len(units) * RING * keys
        bias = []
        for k, (z, d2, s) in enumerate(units):
            if s == 1:
                whole_row(z, d2, 1, pr_sem.at[z * RING + d2])
            at_col = k * RING * keys
            vt[0:hd, at_col : at_col + RING * keys] = (
                g[spot(z, d2, s, 0) : spot(z, d2, s, 0) + RING, keys : 2 * keys, :].reshape(RING * keys, hd).T
            )
            zz = zh if z == 0 else 1 - zh
            cc = core if s == 0 else 1 - core
            for d1 in range(RING):
                dx = lax.rem(x + (1 - cc) * d1 + cc * d2, RING)
                dy = lax.rem(y + cc * d1 + (1 - cc) * d2, RING)
                bias.append(
                    jnp.where(bod_ref[slot_of(dx, zz, dy, cc)] < own_block, 0.0, NEG).astype(F32)
                )

        def scores(i):
            k = jnp.concatenate(
                [
                    g[spot(z, d2, s, 0) : spot(z, d2, s, 0) + RING, 0:keys, :].reshape(RING * keys, hd)
                    for z, d2, s in units
                ],
                axis=0,
            )
            s = lax.dot_general(
                k, qh[i * QB : (i + 1) * QB, :], (((1,), (1,)), ((), ())), preferred_element_type=F32
            )
            parts = []
            for j in range(len(bias)):
                parts.append(s[j * keys : j * keys + anch])
                parts.append(s[j * keys + anch : (j + 1) * keys] + bias[j])
            return jnp.concatenate(parts, axis=0)

        blocks = tok * heads // QB
        s = scores(0)
        for i in range(blocks):
            later = scores(i + 1) if i + 1 < blocks else None
            fold(s, slice(i * QB, (i + 1) * QB), n, False)
            s = later

    pl.semaphore_wait(barrier, 11)
    remote(g.at[spot(0, 0, 0, 0)], g.at[spot(1, 0, 0, 0)], sem(1, 0, 0), "z")
    start_own(0)

    q_load.wait()
    own[...] = q32[...].astype(F32)
    for h in range(heads):
        qh[h * tok : (h + 1) * tok, :] = own[pl.ds(h, tok, stride=heads), :].astype(BF16)
    vt[hd:, :] = jnp.ones((vt.shape[0] - hd, vt.shape[1]), BF16)
    local_pass()

    after_first(0, 3)
    after_first(0, 1)
    after_second(0, 0)
    after_first(0, 2)
    arrived(1, 0, 0)
    start_own(1)
    compute((0, 0, 0))
    after_second(0, 3)
    after_second(0, 1)
    after_second(0, 2)
    after_first(1, 3)
    after_first(1, 1)
    compute((0, 1, 0), (0, 0, 1))
    after_second(1, 0)
    after_first(1, 2)
    after_second_2(0)
    compute((0, 3, 0), (0, 1, 1))
    after_second(1, 3)
    after_second(1, 1)
    compute((1, 0, 0), (0, 3, 1))
    after_second(1, 2)
    compute((0, 2, 0), (1, 0, 1))
    compute((1, 1, 0), (0, 2, 1))
    after_second_2(1)
    compute((1, 3, 0), (1, 1, 1))
    compute((1, 2, 0), (1, 3, 1))
    compute((1, 2, 1))

    for h in range(heads):
        cols = slice(h * tok, (h + 1) * tok)
        at[h * hd : (h + 1) * hd, :] = (
            acc[0:hd, cols] * (1.0 / acc[hd : hd + 1, cols])
        ).astype(BF16)

    side = tp // 2
    u = (1 - side) * tp + side * (3 - tp)

    def real(e):
        return (1 - side) * e + side * (3 - e)

    def pick2(edge, inner):
        return (1 - u) * edge + u * inner

    feats = out_ref.shape[0]
    rows = feats // CHUNKS
    w_load.wait()

    def product(e, ck):
        at_row = pl.multiple_of(e * feats + ck * rows, rows)
        return jnp.dot(w[pl.ds(at_row, rows), :], at[...], preferred_element_type=F32)

    def tp_copy(ph, ck, to, slot):
        r = pl.ds(pl.multiple_of(ck * rows, rows), rows)
        return pltpu.make_async_remote_copy(
            src_ref=sbuf.at[ph, r],
            dst_ref=rbuf.at[slot, r],
            send_sem=ts_sem,
            recv_sem=tr_sem.at[slot * CHUNKS + ck],
            device_id=(ctx, to),
            device_id_type=MESH,
        )

    def landed(slot, ck):
        r = rbuf.at[slot, pl.ds(pl.multiple_of(ck * rows, rows), rows)]
        pltpu.make_async_copy(r, r, tr_sem.at[slot * CHUNKS + ck]).wait()

    plan = (
        (real(pick2(3, 0)), real(pick2(1, 0)), pick2(3, 0)),
        (real(pick2(2, 3)), real(pick2(1, 3)), pick2(2, 1)),
        (real(pick2(1, 2)), real(pick2(1, 2)), pick2(0, 1)),
    )

    def send_block(ph):
        e, to, slot = plan[ph]

        def one(ck, c):
            r = pl.ds(pl.multiple_of(ck * rows, rows), rows)
            if ph == 0:
                sbuf[ph, r, :] = product(e, ck).astype(BF16)
            else:
                part[...] = product(e, ck)

                @pl.when(u == 1)
                def _():
                    landed(4 - ph, ck)
                    part[...] += rbuf[4 - ph, r, :].astype(F32)

                sbuf[ph, r, :] = part[...].astype(BF16)
            tp_copy(ph, ck, to, slot).start()
            return c

        lax.fori_loop(0, CHUNKS, one, 0)

    send_block(0)

    def own_part(ck, c):
        r = pl.ds(pl.multiple_of(ck * rows, rows), rows)
        own[r, :] = product(tp, ck)
        return c

    lax.fori_loop(0, CHUNKS, own_part, 0)
    send_block(1)
    send_block(2)

    def finish(ck, c):
        r = pl.ds(pl.multiple_of(ck * rows, rows), rows)

        landed(0, ck)
        landed(1, ck)
        out_ref[r, :] = (
            own[r, :] + rbuf[0, r, :].astype(F32) + rbuf[1, r, :].astype(F32)
        ).astype(BF16)
        return c

    lax.fori_loop(0, CHUNKS, finish, 0)

    def drain_all():
        gone = g.at[pl.ds(0, len(sent))]
        pltpu.make_async_copy(gone, gone, gs_sem).wait()
        pltpu.make_async_copy(sbuf, sbuf, ts_sem).wait()

    drain_all()


def body(
    queries,
    window_keys,
    window_values,
    anchor_keys,
    anchor_values,
    passing_rows,
    block_of_device,
    out_weight,
):
    tok, heads, hd = queries.shape
    anch = anchor_keys.shape[0]
    ret = passing_rows.shape[1]
    dout = out_weight.shape[0]
    feats = dout // lax.axis_size("tp")
    keys = anch + ret
    n = 2 * RING * keys

    def run(*refs):
        kernel(*refs, tok=tok, heads=heads)

    return pl.pallas_call(
        run,
        out_shape=jax.ShapeDtypeStruct((feats, tok), BF16),
        in_specs=[pl.BlockSpec(memory_space=pltpu.HBM)] * 8,
        out_specs=pl.BlockSpec(memory_space=pltpu.VMEM),
        scratch_shapes=[
            pltpu.VMEM((tok, hd), BF16),
            pltpu.VMEM((tok, hd), BF16),
            pltpu.VMEM((ret, passing_rows.shape[0]), jnp.int32),
            pltpu.SMEM(block_of_device.shape, jnp.int32),
            pltpu.VMEM((HALVES * RING * 2 * RING, 2 * keys, hd), BF16),
            pltpu.VMEM((tok * heads, hd), BF16),
            pltpu.VMEM((tok * heads, hd), BF16),
            pltpu.VMEM(out_weight.shape, BF16),
            pltpu.VMEM((8, tok * heads), F32),
            pltpu.VMEM((hd + 16, tok * heads), F32),
            pltpu.VMEM((hd + 16, n), BF16),
            pltpu.VMEM((heads * hd, tok), BF16),
            pltpu.VMEM((feats, tok), F32),
            pltpu.VMEM((feats // CHUNKS, tok), F32),
            pltpu.VMEM((3, feats, tok), BF16),
            pltpu.VMEM((4, feats, tok), BF16),
            pltpu.SemaphoreType.DMA((8,)),
            pltpu.SemaphoreType.DMA,
            pltpu.SemaphoreType.DMA((26,)),
            pltpu.SemaphoreType.DMA((2 * RING,)),
            pltpu.SemaphoreType.DMA,
            pltpu.SemaphoreType.DMA((4 * CHUNKS,)),
        ],
        compiler_params=pltpu.CompilerParams(
            collective_id=0, has_side_effects=True, vmem_limit_bytes=56_000_000
        ),
        name="layer",
    )(
        *[
            pltpu.with_memory_space_constraint(a, pltpu.HBM)
            for a in (
                window_keys.reshape(tok, hd),
                window_values.reshape(tok, hd),
                anchor_keys.reshape(anch, hd),
                anchor_values.reshape(anch, hd),
                passing_rows.T,
                block_of_device,
                queries.reshape(tok * heads, hd),
                out_weight,
            )
        ]
    )


def solution(mesh):
    return jax.shard_map(
        body,
        mesh=mesh,
        in_specs=(
            P("ctx", "tp", None),
            P("ctx", "tp", None),
            P("ctx", "tp", None),
            P("ctx", "tp", None),
            P("ctx", "tp", None),
            P(),
            P(),
            P(None, "tp"),
        ),
        out_specs=P("tp", "ctx"),
        check_vma=False,
    )
```

```python
import math

import jax
import jax.numpy as jnp
from jax import lax
from jax.experimental import pallas as pl
from jax.experimental.pallas import tpu as pltpu
from jax.sharding import PartitionSpec as P

MESH = pl.DeviceIdType.MESH
RING = 4
HALVES = 2
F32 = jnp.float32
BF16 = jnp.bfloat16
NEG = -1e30
CHUNKS = 4
DIRECT = ((2,), (2,))


def kernel(
    wk_hbm,
    wv_hbm,
    ak_hbm,
    av_hbm,
    prt_hbm,
    bod_hbm,
    q_hbm,
    w_hbm,
    out_ref,
    wk_ref,
    wv_ref,
    prt_ref,
    bod_ref,
    g,
    q32,
    qh,
    w,
    m_ref,
    acc,
    vt,
    at,
    own,
    part,
    sbuf,
    rbuf,
    load_sem,
    gs_sem,
    gr_sem,
    pr_sem,
    ts_sem,
    tr_sem,
    tok,
    heads,
):
    anch = ak_hbm.shape[0]
    ret = prt_ref.shape[0]
    keys = anch + ret
    hd = ak_hbm.shape[1]
    part_tok = tok // 2
    span = part_tok * heads
    ctx = lax.axis_index("ctx")
    tp = lax.axis_index("tp")
    core = lax.rem(ctx, 2)
    y = lax.rem(ctx // 2, RING)
    zh = lax.rem(ctx // (2 * RING), 2)
    x = ctx // (4 * RING)

    def spot(z, d2, s, d1):
        return ((z * RING + d2) * 2 + s) * RING + d1

    def slot_of(xx, zz, yy, cc):
        return ((xx * 2 + zz) * RING + yy) * 2 + cc

    def step_along(first, by):
        dx = core + first - 2 * core * first
        xx = lax.rem(x + (1 - dx) * by + RING, RING)
        yy = lax.rem(y + dx * by + RING, RING)
        return slot_of(xx, zh, yy, core)

    dev = {
        "f+": (step_along(0, 1), tp),
        "f-": (step_along(0, -1), tp),
        "f2": (step_along(0, 2), tp),
        "s+": (step_along(1, 1), tp),
        "s-": (step_along(1, -1), tp),
        "s2": (step_along(1, 2), tp),
        "z": (slot_of(x, 1 - zh, y, core), tp),
        "c": (slot_of(x, zh, y, 1 - core), tp),
    }

    barrier = pltpu.get_barrier_semaphore()
    for d in dev.values():
        pl.semaphore_signal(barrier, inc=1, device_id=d, device_id_type=MESH)
    for k in range(1, 4):
        pl.semaphore_signal(
            barrier, inc=1, device_id=(ctx, lax.rem(tp + k, 4)), device_id_type=MESH
        )

    def load(k, src, dst):
        copy = pltpu.make_async_copy(src, dst, load_sem.at[k])
        copy.start()
        return copy

    prt_load = load(0, prt_hbm, prt_ref)
    wk_load = load(1, wk_hbm, wk_ref)
    wv_load = load(2, wv_hbm, wv_ref)
    ak_load = load(3, ak_hbm, g.at[0, pl.ds(0, anch)])
    av_load = load(4, av_hbm, g.at[0, pl.ds(keys, anch)])
    bod_load = load(5, bod_hbm, bod_ref)
    q_load = load(6, q_hbm, q32)
    w_load = load(7, w_hbm, w)

    prt_load.wait()
    lane = lax.broadcasted_iota(jnp.int32, prt_ref.shape, 1)
    mine = jnp.where(lane == ctx, prt_ref[...], 0).astype(F32)
    chosen = jnp.sum(mine, axis=1, keepdims=True).astype(jnp.int32)
    pick = (lax.broadcasted_iota(jnp.int32, (ret, tok), 1) == chosen).astype(F32).astype(BF16)
    wk_load.wait()
    wv_load.wait()
    g[0, anch:keys, :] = jnp.dot(
        pick, wk_ref[...], preferred_element_type=F32
    ).astype(BF16)
    g[0, keys + anch : 2 * keys, :] = jnp.dot(
        pick, wv_ref[...], preferred_element_type=F32
    ).astype(BF16)

    sent = []

    def remote(src, dst, recv, to):
        copy = pltpu.make_async_remote_copy(
            src_ref=src,
            dst_ref=dst,
            send_sem=gs_sem,
            recv_sem=recv,
            device_id=dev[to],
            device_id_type=MESH,
        )
        copy.start()
        sent.append(1)

    def sem(z, d2, d1):
        return gr_sem.at[z * 13 + (12 if d2 == 2 else d1 + (0, 4, 0, 8)[d2])]

    def arrived(z, d2, d1):
        ref = g.at[spot(z, d2, 0, d1)]
        pltpu.make_async_copy(ref, ref, sem(z, d2, d1)).wait()

    def to_partner(z, d2, d1):
        remote(
            g.at[spot(z, d2, 0, d1)],
            g.at[spot(z, d2, 1, d1)],
            pr_sem.at[z * RING + d2],
            "c",
        )

    def second_all(z, d1):
        own = g.at[spot(z, 0, 0, d1)]
        remote(own, g.at[spot(z, 3, 0, d1)], sem(z, 3, d1), "s+")
        remote(own, g.at[spot(z, 1, 0, d1)], sem(z, 1, d1), "s-")
        if d1 in DIRECT[z]:
            remote(own, g.at[spot(z, 2, 0, d1)], sem(z, 2, d1), "s2")

    def start_own(z):
        own = g.at[spot(z, 0, 0, 0)]
        remote(own, g.at[spot(z, 0, 0, 3)], sem(z, 0, 3), "f+")
        remote(own, g.at[spot(z, 0, 0, 1)], sem(z, 0, 1), "f-")
        remote(own, g.at[spot(z, 0, 0, 2)], sem(z, 0, 2), "f2")
        second_all(z, 0)
        to_partner(z, 0, 0)

    def after_first(z, d1):
        arrived(z, 0, d1)
        second_all(z, d1)
        to_partner(z, 0, d1)

    def after_second(z, d1):
        for d2, to in ((3, "s+"), (1, "s-")):
            arrived(z, d2, d1)
            if d1 not in DIRECT[z] and (d2 == 3) == (d1 in (0, 2)):
                remote(g.at[spot(z, d2, 0, d1)], g.at[spot(z, 2, 0, d1)], sem(z, 2, d1), to)
            to_partner(z, d2, d1)

    def whole_row(z, d2, s, arrival):
        r = g.at[pl.ds(spot(z, d2, s, 0), RING)]
        pltpu.make_async_copy(r, r, arrival).wait()

    def after_second_2(z):
        whole_row(z, 2, 0, sem(z, 2, 0))
        for d1 in range(RING):
            to_partner(z, 2, d1)

    scale = (hd**-0.5) * math.log2(math.e)
    ak_load.wait()
    av_load.wait()
    bod_load.wait()
    own_block = bod_ref[ctx]

    def fold(s, cols, n, first):
        top = jnp.max(s, axis=0, keepdims=True)
        if first:
            new = top
        else:
            old = m_ref[0:1, cols]
            new = jnp.maximum(old, top)
        p = jnp.exp2((s - new) * scale).astype(BF16)
        add = jnp.dot(vt[:, 0:n], p, preferred_element_type=F32)
        if first:
            acc[:, cols] = add
        else:
            acc[:, cols] = acc[:, cols] * jnp.exp2((old - new) * scale) + add
        m_ref[0:1, cols] = new

    def local_pass():
        vt[0:hd, 0:tok] = wv_ref[...].T
        row = lax.broadcasted_iota(jnp.int32, (tok, span), 0)
        col = lax.broadcasted_iota(jnp.int32, (tok, span), 1)
        place = lax.rem(col, part_tok)

        def scores(cols, p):
            s = lax.dot_general(
                wk_ref[...], qh[cols, :], (((1,), (1,)), ((), ())), preferred_element_type=F32
            )
            return jnp.where(row <= place + p * part_tok, s, NEG)

        first, second = slice(0, span), slice(span, 2 * span)
        s, later = scores(first, 0), scores(second, 1)
        fold(s, first, tok, True)
        fold(later, second, tok, True)

    waited = set()

    both = (slice(0, span), slice(span, 2 * span))
    early = (slice(0, span // 2), slice(span // 2, span))
    late = (slice(span, 3 * span // 2), slice(3 * span // 2, 2 * span))

    def compute(*units, blocks=both):
        n = len(units) * RING * keys
        bias = []
        for k, (z, d2, s) in enumerate(units):
            if s == 1 and (z, d2) not in waited:
                waited.add((z, d2))
                whole_row(z, d2, 1, pr_sem.at[z * RING + d2])
            at_col = k * RING * keys
            vt[0:hd, at_col : at_col + RING * keys] = (
                g[spot(z, d2, s, 0) : spot(z, d2, s, 0) + RING, keys : 2 * keys, :].reshape(RING * keys, hd).T
            )
            zz = zh if z == 0 else 1 - zh
            cc = core if s == 0 else 1 - core
            for d1 in range(RING):
                dx = lax.rem(x + (1 - cc) * d1 + cc * d2, RING)
                dy = lax.rem(y + cc * d1 + (1 - cc) * d2, RING)
                bias.append(
                    jnp.where(bod_ref[slot_of(dx, zz, dy, cc)] < own_block, 0.0, NEG).astype(F32)
                )

        def scores(cols):
            k = jnp.concatenate(
                [
                    g[spot(z, d2, s, 0) : spot(z, d2, s, 0) + RING, 0:keys, :].reshape(RING * keys, hd)
                    for z, d2, s in units
                ],
                axis=0,
            )
            s = lax.dot_general(
                k, qh[cols, :], (((1,), (1,)), ((), ())), preferred_element_type=F32
            )
            parts = []
            for j in range(len(bias)):
                parts.append(s[j * keys : j * keys + anch])
                parts.append(s[j * keys + anch : (j + 1) * keys] + bias[j])
            return jnp.concatenate(parts, axis=0)

        s = scores(blocks[0])
        for i, cols in enumerate(blocks):
            later = scores(blocks[i + 1]) if i + 1 < len(blocks) else None
            fold(s, cols, n, False)
            s = later

    pl.semaphore_wait(barrier, 11)
    remote(g.at[spot(0, 0, 0, 0)], g.at[spot(1, 0, 0, 0)], sem(1, 0, 0), "z")
    start_own(0)

    q_load.wait()
    own[...] = q32[...].astype(F32)
    for h in range(heads):
        of_head = own[pl.ds(h, tok, stride=heads), :].astype(BF16)
        for p in range(2):
            row = p * span + h * part_tok
            qh[row : row + part_tok, :] = of_head[p * part_tok : (p + 1) * part_tok]
    vt[hd:, :] = jnp.ones((vt.shape[0] - hd, vt.shape[1]), BF16)
    local_pass()

    after_first(0, 3)
    after_first(0, 1)
    after_second(0, 0)
    after_first(0, 2)
    arrived(1, 0, 0)
    start_own(1)
    compute((0, 0, 0))
    after_second(0, 3)
    after_second(0, 1)
    after_second(0, 2)
    after_first(1, 3)
    after_first(1, 1)
    compute((0, 1, 0), (0, 0, 1))
    after_second(1, 0)
    after_first(1, 2)
    after_second_2(0)
    compute((0, 3, 0), (0, 1, 1))
    after_second(1, 3)
    after_second(1, 1)
    compute((1, 0, 0), (0, 3, 1))
    after_second(1, 2)
    compute((0, 2, 0), (1, 0, 1))
    compute((1, 1, 0), (0, 2, 1), blocks=early)
    after_second_2(1)
    compute((1, 3, 0), (1, 1, 1), blocks=early)
    compute((1, 2, 0), (1, 3, 1), blocks=early)
    compute((1, 2, 1), blocks=early)

    low = lax.broadcasted_iota(jnp.int32, (hd, 2 * part_tok), 1) < part_tok

    def normalize(p):
        for h in range(0, heads, 2):
            cols = slice(p * span + h * part_tok, p * span + (h + 2) * part_tok)
            pair = acc[0:hd, cols] * (1.0 / acc[hd : hd + 1, cols])
            turned = pltpu.roll(pair, part_tok, 1)
            for k, (lo, hi) in enumerate(((pair, turned), (turned, pair))):
                rows = slice((h + k) * hd, (h + k + 1) * hd)
                at[p, 0, rows, :] = jnp.where(low, lo, 0.0).astype(BF16)
                at[p, 1, rows, :] = jnp.where(low, 0.0, hi).astype(BF16)

    normalize(0)

    side = tp // 2
    u = (1 - side) * tp + side * (3 - tp)

    def real(e):
        return (1 - side) * e + side * (3 - e)

    def pick2(edge, inner):
        return (1 - u) * edge + u * inner

    feats = out_ref.shape[0]
    rows = feats // CHUNKS
    w_load.wait()

    def product(e, p, cc):
        at_row = pl.multiple_of(e * feats + cc * 2 * rows, rows)
        return jnp.dot(
            w[pl.ds(at_row, rows), :], at[p, p], preferred_element_type=F32
        ) + jnp.dot(
            w[pl.ds(at_row + rows, rows), :], at[p, 1 - p], preferred_element_type=F32
        )

    def tp_copy(ph, ck, to, slot):
        r = pl.ds(pl.multiple_of(ck * rows, rows), rows)
        return pltpu.make_async_remote_copy(
            src_ref=sbuf.at[ph, r],
            dst_ref=rbuf.at[slot, r],
            send_sem=ts_sem,
            recv_sem=tr_sem.at[slot * CHUNKS + ck],
            device_id=(ctx, to),
            device_id_type=MESH,
        )

    def landed(slot, ck):
        r = rbuf.at[slot, pl.ds(pl.multiple_of(ck * rows, rows), rows)]
        pltpu.make_async_copy(r, r, tr_sem.at[slot * CHUNKS + ck]).wait()

    plan = (
        (real(pick2(3, 0)), real(pick2(1, 0)), pick2(3, 0)),
        (real(pick2(2, 3)), real(pick2(1, 3)), pick2(2, 1)),
        (real(pick2(1, 2)), real(pick2(1, 2)), pick2(0, 1)),
    )

    per = CHUNKS // 2

    def send_block(ph, p):
        e, to, slot = plan[ph]

        def one(cc, c):
            ck = p * per + cc
            r = pl.ds(pl.multiple_of(ck * rows, rows), rows)
            if ph == 0:
                sbuf[ph, r, :] = product(e, p, cc).astype(BF16)
            else:
                part[...] = product(e, p, cc)

                @pl.when(u == 1)
                def _():
                    landed(4 - ph, ck)
                    part[...] += rbuf[4 - ph, r, :].astype(F32)

                sbuf[ph, r, :] = part[...].astype(BF16)
            tp_copy(ph, ck, to, slot).start()
            return c

        lax.fori_loop(0, per, one, 0)

    def own_part(p):
        def one(cc, c):
            r = pl.ds(pl.multiple_of((p * per + cc) * rows, rows), rows)
            own[r, :] = product(tp, p, cc)
            return c

        lax.fori_loop(0, per, one, 0)

    send_block(0, 0)
    pl.when(u == 0)(lambda: send_block(1, 0))
    compute((1, 1, 0), (0, 2, 1), (1, 3, 0), (1, 1, 1), blocks=late)
    compute((1, 2, 0), (1, 3, 1), (1, 2, 1), blocks=late)
    normalize(1)
    send_block(0, 1)
    own_part(0)
    pl.when(u == 1)(lambda: send_block(1, 0))
    own_part(1)
    send_block(1, 1)
    send_block(2, 0)
    send_block(2, 1)

    first_half = lax.broadcasted_iota(jnp.int32, (rows, tok), 1) < part_tok

    def summed(ck):
        r = pl.ds(pl.multiple_of(ck * rows, rows), rows)

        landed(0, ck)
        landed(1, ck)
        return own[r, :] + rbuf[0, r, :].astype(F32) + rbuf[1, r, :].astype(F32)

    def finish():
        def one(cc, c):
            here, there = summed(cc), summed(per + cc)
            r = pl.multiple_of(cc * 2 * rows, rows)
            out_ref[pl.ds(r, rows), :] = jnp.where(first_half, here, there).astype(BF16)
            out_ref[pl.ds(r + rows, rows), :] = pltpu.roll(
                jnp.where(first_half, there, here), part_tok, 1
            ).astype(BF16)
            return c

        lax.fori_loop(0, per, one, 0)

    finish()

    def drain_all():
        gone = g.at[pl.ds(0, len(sent))]
        pltpu.make_async_copy(gone, gone, gs_sem).wait()
        pltpu.make_async_copy(sbuf, sbuf, ts_sem).wait()

    drain_all()


def body(
    queries,
    window_keys,
    window_values,
    anchor_keys,
    anchor_values,
    passing_rows,
    block_of_device,
    out_weight,
):
    tok, heads, hd = queries.shape
    anch = anchor_keys.shape[0]
    ret = passing_rows.shape[1]
    dout = out_weight.shape[0]
    feats = dout // lax.axis_size("tp")
    keys = anch + ret
    n = 4 * RING * keys

    def run(*refs):
        kernel(*refs, tok=tok, heads=heads)

    return pl.pallas_call(
        run,
        out_shape=jax.ShapeDtypeStruct((feats, tok), BF16),
        in_specs=[pl.BlockSpec(memory_space=pltpu.HBM)] * 8,
        out_specs=pl.BlockSpec(memory_space=pltpu.VMEM),
        scratch_shapes=[
            pltpu.VMEM((tok, hd), BF16),
            pltpu.VMEM((tok, hd), BF16),
            pltpu.VMEM((ret, passing_rows.shape[0]), jnp.int32),
            pltpu.SMEM(block_of_device.shape, jnp.int32),
            pltpu.VMEM((HALVES * RING * 2 * RING, 2 * keys, hd), BF16),
            pltpu.VMEM((tok * heads, hd), BF16),
            pltpu.VMEM((tok * heads, hd), BF16),
            pltpu.VMEM(out_weight.shape, BF16),
            pltpu.VMEM((8, tok * heads), F32),
            pltpu.VMEM((hd + 16, tok * heads), F32),
            pltpu.VMEM((hd + 16, n), BF16),
            pltpu.VMEM((2, 2, heads * hd, tok), BF16),
            pltpu.VMEM((feats, tok), F32),
            pltpu.VMEM((feats // CHUNKS, tok), F32),
            pltpu.VMEM((3, feats, tok), BF16),
            pltpu.VMEM((4, feats, tok), BF16),
            pltpu.SemaphoreType.DMA((8,)),
            pltpu.SemaphoreType.DMA,
            pltpu.SemaphoreType.DMA((26,)),
            pltpu.SemaphoreType.DMA((2 * RING,)),
            pltpu.SemaphoreType.DMA,
            pltpu.SemaphoreType.DMA((4 * CHUNKS,)),
        ],
        compiler_params=pltpu.CompilerParams(
            collective_id=0, has_side_effects=True, vmem_limit_bytes=56_000_000
        ),
        name="layer",
    )(
        *[
            pltpu.with_memory_space_constraint(a, pltpu.HBM)
            for a in (
                window_keys.reshape(tok, hd),
                window_values.reshape(tok, hd),
                anchor_keys.reshape(anch, hd),
                anchor_values.reshape(anch, hd),
                passing_rows.T,
                block_of_device,
                queries.reshape(tok * heads, hd),
                out_weight,
            )
        ]
    )


def solution(mesh):
    return jax.shard_map(
        body,
        mesh=mesh,
        in_specs=(
            P("ctx", "tp", None),
            P("ctx", "tp", None),
            P("ctx", "tp", None),
            P("ctx", "tp", None),
            P("ctx", "tp", None),
            P(),
            P(),
            P(None, "tp"),
        ),
        out_specs=P("tp", "ctx"),
        check_vma=False,
    )
```

```python
import math

import jax
import jax.numpy as jnp
from jax import lax
from jax.experimental import pallas as pl
from jax.experimental.pallas import tpu as pltpu
from jax.sharding import PartitionSpec as P

MESH = pl.DeviceIdType.MESH
RING = 4
HALVES = 2
F32 = jnp.float32
BF16 = jnp.bfloat16
NEG = -1e30
CHUNKS = 4
DIRECT = ((2,), (2,))


def kernel(
    wk_hbm,
    wv_hbm,
    ak_hbm,
    av_hbm,
    prt_hbm,
    bod_hbm,
    q_hbm,
    w_hbm,
    out_ref,
    wk_ref,
    wv_ref,
    prt_ref,
    bod_ref,
    g,
    q32,
    qh,
    w,
    m_ref,
    acc,
    vt,
    at,
    own,
    part,
    sbuf,
    rbuf,
    load_sem,
    gs_sem,
    gr_sem,
    pr_sem,
    ts_sem,
    tr_sem,
    tok,
    heads,
):
    anch = ak_hbm.shape[0]
    ret = prt_ref.shape[0]
    keys = anch + ret
    hd = ak_hbm.shape[1]
    part_tok = tok // 2
    span = part_tok * heads
    ctx = lax.axis_index("ctx")
    tp = lax.axis_index("tp")
    core = lax.rem(ctx, 2)
    y = lax.rem(ctx // 2, RING)
    zh = lax.rem(ctx // (2 * RING), 2)
    x = ctx // (4 * RING)

    def spot(z, d2, s, d1):
        return ((z * RING + d2) * 2 + s) * RING + d1

    def slot_of(xx, zz, yy, cc):
        return ((xx * 2 + zz) * RING + yy) * 2 + cc

    def step_along(first, by):
        dx = core + first - 2 * core * first
        xx = lax.rem(x + (1 - dx) * by + RING, RING)
        yy = lax.rem(y + dx * by + RING, RING)
        return slot_of(xx, zh, yy, core)

    dev = {
        "f+": (step_along(0, 1), tp),
        "f-": (step_along(0, -1), tp),
        "f2": (step_along(0, 2), tp),
        "s+": (step_along(1, 1), tp),
        "s-": (step_along(1, -1), tp),
        "s2": (step_along(1, 2), tp),
        "z": (slot_of(x, 1 - zh, y, core), tp),
        "c": (slot_of(x, zh, y, 1 - core), tp),
    }

    barrier = pltpu.get_barrier_semaphore()
    for d in dev.values():
        pl.semaphore_signal(barrier, inc=1, device_id=d, device_id_type=MESH)
    for k in range(1, 4):
        pl.semaphore_signal(
            barrier, inc=1, device_id=(ctx, lax.rem(tp + k, 4)), device_id_type=MESH
        )

    def load(k, src, dst):
        copy = pltpu.make_async_copy(src, dst, load_sem.at[k])
        copy.start()
        return copy

    prt_load = load(0, prt_hbm, prt_ref)
    wk_load = load(1, wk_hbm, wk_ref)
    wv_load = load(2, wv_hbm, wv_ref)
    ak_load = load(3, ak_hbm, g.at[0, pl.ds(0, anch)])
    av_load = load(4, av_hbm, g.at[0, pl.ds(keys, anch)])
    bod_load = load(5, bod_hbm, bod_ref)
    q_load = load(6, q_hbm, q32)
    w_load = load(7, w_hbm, w)

    prt_load.wait()
    lane = lax.broadcasted_iota(jnp.int32, prt_ref.shape, 1)
    mine = jnp.where(lane == ctx, prt_ref[...], 0).astype(F32)
    chosen = jnp.sum(mine, axis=1, keepdims=True).astype(jnp.int32)
    pick = (lax.broadcasted_iota(jnp.int32, (ret, tok), 1) == chosen).astype(F32).astype(BF16)
    wk_load.wait()
    wv_load.wait()
    g[0, anch:keys, :] = jnp.dot(
        pick, wk_ref[...], preferred_element_type=F32
    ).astype(BF16)
    g[0, keys + anch : 2 * keys, :] = jnp.dot(
        pick, wv_ref[...], preferred_element_type=F32
    ).astype(BF16)

    sent = []

    def remote(src, dst, recv, to):
        copy = pltpu.make_async_remote_copy(
            src_ref=src,
            dst_ref=dst,
            send_sem=gs_sem,
            recv_sem=recv,
            device_id=dev[to],
            device_id_type=MESH,
        )
        copy.start()
        sent.append(1)

    def sem(z, d2, d1):
        return gr_sem.at[z * 13 + (12 if d2 == 2 else d1 + (0, 4, 0, 8)[d2])]

    def arrived(z, d2, d1):
        ref = g.at[spot(z, d2, 0, d1)]
        pltpu.make_async_copy(ref, ref, sem(z, d2, d1)).wait()

    def to_partner(z, d2, d1):
        remote(
            g.at[spot(z, d2, 0, d1)],
            g.at[spot(z, d2, 1, d1)],
            pr_sem.at[z * RING + d2],
            "c",
        )

    def second_all(z, d1):
        own = g.at[spot(z, 0, 0, d1)]
        remote(own, g.at[spot(z, 3, 0, d1)], sem(z, 3, d1), "s+")
        remote(own, g.at[spot(z, 1, 0, d1)], sem(z, 1, d1), "s-")
        if d1 in DIRECT[z]:
            remote(own, g.at[spot(z, 2, 0, d1)], sem(z, 2, d1), "s2")

    def start_own(z):
        own = g.at[spot(z, 0, 0, 0)]
        remote(own, g.at[spot(z, 0, 0, 3)], sem(z, 0, 3), "f+")
        remote(own, g.at[spot(z, 0, 0, 1)], sem(z, 0, 1), "f-")
        remote(own, g.at[spot(z, 0, 0, 2)], sem(z, 0, 2), "f2")
        second_all(z, 0)
        to_partner(z, 0, 0)

    def after_first(z, d1):
        arrived(z, 0, d1)
        second_all(z, d1)
        to_partner(z, 0, d1)

    def after_second(z, d1):
        for d2, to in ((3, "s+"), (1, "s-")):
            arrived(z, d2, d1)
            if d1 not in DIRECT[z] and (d2 == 3) == (d1 in (0, 2)):
                remote(g.at[spot(z, d2, 0, d1)], g.at[spot(z, 2, 0, d1)], sem(z, 2, d1), to)
            to_partner(z, d2, d1)

    def whole_row(z, d2, s, arrival):
        r = g.at[pl.ds(spot(z, d2, s, 0), RING)]
        pltpu.make_async_copy(r, r, arrival).wait()

    def after_second_2(z):
        whole_row(z, 2, 0, sem(z, 2, 0))
        for d1 in range(RING):
            to_partner(z, 2, d1)

    scale = (hd**-0.5) * math.log2(math.e)
    ak_load.wait()
    av_load.wait()
    bod_load.wait()
    own_block = bod_ref[ctx]

    def twice(k):
        return jnp.concatenate([k, k], axis=1)

    def fold(s, cols, n, first):
        top = jnp.max(s, axis=0, keepdims=True)
        if first:
            new = top
        else:
            old = m_ref[0:1, cols]
            new = jnp.maximum(old, top)
        p = jnp.exp2(s - new).astype(BF16)
        add = jnp.dot(vt[:, 0:n], p, preferred_element_type=F32)
        if first:
            acc[:, cols] = add
        else:
            acc[:, cols] = acc[:, cols] * jnp.exp2(old - new) + add
        m_ref[0:1, cols] = new

    def local_pass():
        vt[0:hd, 0:tok] = wv_ref[...].T
        row = lax.broadcasted_iota(jnp.int32, (tok, span), 0)
        col = lax.broadcasted_iota(jnp.int32, (tok, span), 1)
        place = lax.rem(col, part_tok)

        def scores(cols, p):
            s = lax.dot_general(
                twice(wk_ref[...]), qh[cols, :], (((1,), (1,)), ((), ())), preferred_element_type=F32
            )
            return jnp.where(row <= place + p * part_tok, s, NEG)

        first, second = slice(0, span), slice(span, 2 * span)
        s, later = scores(first, 0), scores(second, 1)
        fold(s, first, tok, True)
        fold(later, second, tok, True)

    waited = set()

    both = (slice(0, span), slice(span, 2 * span))
    early = (slice(0, span // 2), slice(span // 2, span))
    late = (slice(span, 3 * span // 2), slice(3 * span // 2, 2 * span))

    def compute(*units, blocks=both):
        n = len(units) * RING * keys
        bias = []
        for k, (z, d2, s) in enumerate(units):
            if s == 1 and (z, d2) not in waited:
                waited.add((z, d2))
                whole_row(z, d2, 1, pr_sem.at[z * RING + d2])
            at_col = k * RING * keys
            vt[0:hd, at_col : at_col + RING * keys] = (
                g[spot(z, d2, s, 0) : spot(z, d2, s, 0) + RING, keys : 2 * keys, :].reshape(RING * keys, hd).T
            )
            zz = zh if z == 0 else 1 - zh
            cc = core if s == 0 else 1 - core
            for d1 in range(RING):
                dx = lax.rem(x + (1 - cc) * d1 + cc * d2, RING)
                dy = lax.rem(y + cc * d1 + (1 - cc) * d2, RING)
                bias.append(
                    jnp.where(bod_ref[slot_of(dx, zz, dy, cc)] < own_block, 0.0, NEG).astype(F32)
                )

        def scores(cols):
            k = jnp.concatenate(
                [
                    g[spot(z, d2, s, 0) : spot(z, d2, s, 0) + RING, 0:keys, :].reshape(RING * keys, hd)
                    for z, d2, s in units
                ],
                axis=0,
            )
            s = lax.dot_general(
                twice(k), qh[cols, :], (((1,), (1,)), ((), ())), preferred_element_type=F32
            )
            parts = []
            for j in range(len(bias)):
                parts.append(s[j * keys : j * keys + anch])
                parts.append(s[j * keys + anch : (j + 1) * keys] + bias[j])
            return jnp.concatenate(parts, axis=0)

        s = scores(blocks[0])
        for i, cols in enumerate(blocks):
            later = scores(blocks[i + 1]) if i + 1 < len(blocks) else None
            fold(s, cols, n, False)
            s = later

    pl.semaphore_wait(barrier, 11)
    remote(g.at[spot(0, 0, 0, 0)], g.at[spot(1, 0, 0, 0)], sem(1, 0, 0), "z")
    start_own(0)

    q_load.wait()
    own[...] = q32[...].astype(F32)
    for h in range(heads):
        exact = own[pl.ds(h, tok, stride=heads), :] * scale
        high = exact.astype(BF16)
        low_bits = (exact - high.astype(F32)).astype(BF16)
        for p in range(2):
            row = p * span + h * part_tok
            mine = slice(p * part_tok, (p + 1) * part_tok)
            qh[row : row + part_tok, 0:hd] = high[mine]
            qh[row : row + part_tok, hd:] = low_bits[mine]
    vt[hd:, :] = jnp.ones((vt.shape[0] - hd, vt.shape[1]), BF16)
    local_pass()

    after_first(0, 3)
    after_first(0, 1)
    after_second(0, 0)
    after_first(0, 2)
    arrived(1, 0, 0)
    start_own(1)
    compute((0, 0, 0))
    after_second(0, 3)
    after_second(0, 1)
    after_second(0, 2)
    after_first(1, 3)
    after_first(1, 1)
    compute((0, 1, 0), (0, 0, 1))
    after_second(1, 0)
    after_first(1, 2)
    after_second_2(0)
    compute((0, 3, 0), (0, 1, 1))
    after_second(1, 3)
    after_second(1, 1)
    compute((1, 0, 0), (0, 3, 1))
    after_second(1, 2)
    compute((0, 2, 0), (1, 0, 1))
    compute((1, 1, 0), (0, 2, 1), blocks=early)
    after_second_2(1)
    compute((1, 3, 0), (1, 1, 1), blocks=early)
    compute((1, 2, 0), (1, 3, 1), blocks=early)
    compute((1, 2, 1), blocks=early)

    low = lax.broadcasted_iota(jnp.int32, (hd, 2 * part_tok), 1) < part_tok

    def normalize(p):
        for h in range(0, heads, 2):
            cols = slice(p * span + h * part_tok, p * span + (h + 2) * part_tok)
            pair = acc[0:hd, cols] * (1.0 / acc[hd : hd + 1, cols])
            turned = pltpu.roll(pair, part_tok, 1)
            for k, (lo, hi) in enumerate(((pair, turned), (turned, pair))):
                rows = slice((h + k) * hd, (h + k + 1) * hd)
                at[p, 0, rows, :] = jnp.where(low, lo, 0.0).astype(BF16)
                at[p, 1, rows, :] = jnp.where(low, 0.0, hi).astype(BF16)

    normalize(0)

    side = tp // 2
    u = (1 - side) * tp + side * (3 - tp)

    def real(e):
        return (1 - side) * e + side * (3 - e)

    def pick2(edge, inner):
        return (1 - u) * edge + u * inner

    feats = out_ref.shape[0]
    rows = feats // CHUNKS
    w_load.wait()

    def product(e, p, cc):
        at_row = pl.multiple_of(e * feats + cc * 2 * rows, rows)
        return jnp.dot(
            w[pl.ds(at_row, rows), :], at[p, p], preferred_element_type=F32
        ) + jnp.dot(
            w[pl.ds(at_row + rows, rows), :], at[p, 1 - p], preferred_element_type=F32
        )

    def tp_copy(ph, ck, to, slot):
        r = pl.ds(pl.multiple_of(ck * rows, rows), rows)
        return pltpu.make_async_remote_copy(
            src_ref=sbuf.at[ph, r],
            dst_ref=rbuf.at[slot, r],
            send_sem=ts_sem,
            recv_sem=tr_sem.at[slot * CHUNKS + ck],
            device_id=(ctx, to),
            device_id_type=MESH,
        )

    def landed(slot, ck):
        r = rbuf.at[slot, pl.ds(pl.multiple_of(ck * rows, rows), rows)]
        pltpu.make_async_copy(r, r, tr_sem.at[slot * CHUNKS + ck]).wait()

    plan = (
        (real(pick2(3, 0)), real(pick2(1, 0)), pick2(3, 0)),
        (real(pick2(2, 3)), real(pick2(1, 3)), pick2(2, 1)),
        (real(pick2(1, 2)), real(pick2(1, 2)), pick2(0, 1)),
    )

    per = CHUNKS // 2

    def send_block(ph, p):
        e, to, slot = plan[ph]

        def one(cc, c):
            ck = p * per + cc
            r = pl.ds(pl.multiple_of(ck * rows, rows), rows)
            if ph == 0:
                sbuf[ph, r, :] = product(e, p, cc).astype(BF16)
            else:
                part[...] = product(e, p, cc)

                @pl.when(u == 1)
                def _():
                    landed(4 - ph, ck)
                    part[...] += rbuf[4 - ph, r, :].astype(F32)

                sbuf[ph, r, :] = part[...].astype(BF16)
            tp_copy(ph, ck, to, slot).start()
            return c

        lax.fori_loop(0, per, one, 0)

    def own_part(p):
        def one(cc, c):
            r = pl.ds(pl.multiple_of((p * per + cc) * rows, rows), rows)
            own[r, :] = product(tp, p, cc)
            return c

        lax.fori_loop(0, per, one, 0)

    send_block(0, 0)
    pl.when(u == 0)(lambda: send_block(1, 0))
    compute((1, 1, 0), (0, 2, 1), (1, 3, 0), (1, 1, 1), blocks=late)
    compute((1, 2, 0), (1, 3, 1), (1, 2, 1), blocks=late)
    normalize(1)
    send_block(0, 1)
    own_part(0)
    pl.when(u == 1)(lambda: send_block(1, 0))
    own_part(1)
    send_block(1, 1)
    send_block(2, 0)
    send_block(2, 1)

    first_half = lax.broadcasted_iota(jnp.int32, (rows, tok), 1) < part_tok

    def summed(ck):
        r = pl.ds(pl.multiple_of(ck * rows, rows), rows)

        landed(0, ck)
        landed(1, ck)
        return own[r, :] + rbuf[0, r, :].astype(F32) + rbuf[1, r, :].astype(F32)

    def finish():
        def one(cc, c):
            here, there = summed(cc), summed(per + cc)
            r = pl.multiple_of(cc * 2 * rows, rows)
            out_ref[pl.ds(r, rows), :] = jnp.where(first_half, here, there).astype(BF16)
            out_ref[pl.ds(r + rows, rows), :] = pltpu.roll(
                jnp.where(first_half, there, here), part_tok, 1
            ).astype(BF16)
            return c

        lax.fori_loop(0, per, one, 0)

    finish()

    def drain_all():
        gone = g.at[pl.ds(0, len(sent))]
        pltpu.make_async_copy(gone, gone, gs_sem).wait()
        pltpu.make_async_copy(sbuf, sbuf, ts_sem).wait()

    drain_all()


def body(
    queries,
    window_keys,
    window_values,
    anchor_keys,
    anchor_values,
    passing_rows,
    block_of_device,
    out_weight,
):
    tok, heads, hd = queries.shape
    anch = anchor_keys.shape[0]
    ret = passing_rows.shape[1]
    dout = out_weight.shape[0]
    feats = dout // lax.axis_size("tp")
    keys = anch + ret
    n = 4 * RING * keys

    def run(*refs):
        kernel(*refs, tok=tok, heads=heads)

    return pl.pallas_call(
        run,
        out_shape=jax.ShapeDtypeStruct((feats, tok), BF16),
        in_specs=[pl.BlockSpec(memory_space=pltpu.HBM)] * 8,
        out_specs=pl.BlockSpec(memory_space=pltpu.VMEM),
        scratch_shapes=[
            pltpu.VMEM((tok, hd), BF16),
            pltpu.VMEM((tok, hd), BF16),
            pltpu.VMEM((ret, passing_rows.shape[0]), jnp.int32),
            pltpu.SMEM(block_of_device.shape, jnp.int32),
            pltpu.VMEM((HALVES * RING * 2 * RING, 2 * keys, hd), BF16),
            pltpu.VMEM((tok * heads, hd), BF16),
            pltpu.VMEM((tok * heads, 2 * hd), BF16),
            pltpu.VMEM(out_weight.shape, BF16),
            pltpu.VMEM((8, tok * heads), F32),
            pltpu.VMEM((hd + 16, tok * heads), F32),
            pltpu.VMEM((hd + 16, n), BF16),
            pltpu.VMEM((2, 2, heads * hd, tok), BF16),
            pltpu.VMEM((feats, tok), F32),
            pltpu.VMEM((feats // CHUNKS, tok), F32),
            pltpu.VMEM((3, feats, tok), BF16),
            pltpu.VMEM((4, feats, tok), BF16),
            pltpu.SemaphoreType.DMA((8,)),
            pltpu.SemaphoreType.DMA,
            pltpu.SemaphoreType.DMA((26,)),
            pltpu.SemaphoreType.DMA((2 * RING,)),
            pltpu.SemaphoreType.DMA,
            pltpu.SemaphoreType.DMA((4 * CHUNKS,)),
        ],
        compiler_params=pltpu.CompilerParams(
            collective_id=0, has_side_effects=True, vmem_limit_bytes=56_000_000
        ),
        name="layer",
    )(
        *[
            pltpu.with_memory_space_constraint(a, pltpu.HBM)
            for a in (
                window_keys.reshape(tok, hd),
                window_values.reshape(tok, hd),
                anchor_keys.reshape(anch, hd),
                anchor_values.reshape(anch, hd),
                passing_rows.T,
                block_of_device,
                queries.reshape(tok * heads, hd),
                out_weight,
            )
        ]
    )


def solution(mesh):
    return jax.shard_map(
        body,
        mesh=mesh,
        in_specs=(
            P("ctx", "tp", None),
            P("ctx", "tp", None),
            P("ctx", "tp", None),
            P("ctx", "tp", None),
            P("ctx", "tp", None),
            P(),
            P(),
            P(None, "tp"),
        ),
        out_specs=P("tp", "ctx"),
        check_vma=False,
    )
```
